32 devices in a mesh: seq: 16 (over z, y, x), head: 2 (over core).
Axes of the slice: x: 2, y: 2, z: 4, core: 2. Of those that a mesh axis runs over, the one named last changes fastest.
Arguments:
- queries: bfloat16 [4096, 32, 128], P('seq', 'head'), may hold values from -8 to 8
- keys: bfloat16 [4096, 8, 128], P('seq', 'head'), may hold values from -8 to 8
- values: bfloat16 [4096, 8, 128], P('seq', 'head'), may hold values from -6 to 6
- out_weight: bfloat16 [4096, 4096], P('head', 'seq'), may hold values from -0.125 to 0.125
- doc_lengths: int32 [16], replicated, may hold values from 1 to 2304, 4096 in all
Outputs:
- projected: bfloat16 [4096, 4096], P('seq', 'head')
The draws below stay inside these ranges and needn't reach their ends.
Inputs may be any that keep to these rules, and one draw needn't show every extreme that they name: `doc_lengths`: every document is at most 2304 tokens long and the longest is exactly that; the lengths sum to 4096.
All inputs are finite; a program needn't handle non-finite values.
Results may differ from the reference program's by a relative error of at most 0.014.
Values may be sent and summed in bfloat16 or wider, within the bound.
A program may use at most 64 MiB of HBM per device.

```python
import math
import jax
import jax.numpy as jnp
import numpy as np
from jax import lax

D = 4096
H = 32
KVH = 8
HD = 128
TOK_DEV = 256
REACH = 9
TOKENS = 4096
NDOCS = 16
N_HEAD = 2


def drawn_draws(base_key):
    first_key, second_key = jax.random.split(base_key, 2)
    queries = jnp.clip(jax.random.normal(first_key, (TOKENS, H, HD)), -8.0, 8.0)
    keys = jnp.clip(jax.random.normal(second_key, (TOKENS, KVH, HD)), -8.0, 8.0)
    return (queries, keys)


def draw_queries(key, part):
    queries, keys = drawn_draws(jax.random.fold_in(key, 7))
    return queries.astype(jnp.bfloat16)


def draw_keys(key, part):
    queries, keys = drawn_draws(jax.random.fold_in(key, 7))
    return keys.astype(jnp.bfloat16)


def with_spikes(result, own_key, source, target, blocks, factor):
    owner, partner = [(jnp.arange(result.shape[dim]) // (result.shape[dim] // blocks)).reshape([-1 if axis == dim else 1 for axis in range(result.ndim)]) for dim in (source, target)]
    chosen = jax.random.permutation(own_key, blocks)[partner]
    strong = (owner == chosen) | (owner == (partner + blocks // 2) % blocks)
    return jnp.where(strong, factor * result, result)


def shard_levels(own_key, dims, pieces, smallest, largest):
    gain = 1.0
    for dim, parts in pieces:
        draws = jax.random.uniform(jax.random.fold_in(jax.random.fold_in(own_key, 6), dim), (parts,), jnp.float32, smallest / len(pieces), largest / len(pieces))
        gain = gain * jnp.repeat(jnp.exp(draws), dims[dim] // parts).reshape((-1,) + (1,) * (len(dims) - 1 - dim))
    return gain


def length_profile(count, total, bound, lean):
    portions = [(1 << 20) // math.isqrt(standing ** lean) + 1 for standing in range(2, count + 1)]
    spare, given = total - bound - (count - 1), [1] * (count - 1)
    while spare > 0:
        candidates = [i for i in range(count - 1) if given[i] < bound]
        mass, remaining = sum([portions[i] for i in candidates]), spare
        for i in candidates:
            extra = min(bound - given[i], max(1, remaining * portions[i] // mass), spare)
            given[i] = given[i] + extra
            spare = spare - extra
    return np.array([bound] + given)


def uneven_parts(key, count, total, most, lean):
    if count == 2:
        one = jax.random.randint(key, (), max(1, total - most), min(most, total - 1) + 1)
        return jnp.stack([one, total - one])
    sizes = jnp.asarray(length_profile(count, total, most, lean), jnp.int32)
    twos = (count - 1) // 2
    donor, taker = sizes[1:1 + 2 * twos:2], sizes[2:2 + 2 * twos:2]
    room = jnp.minimum(donor - 1, most - taker)
    passed = jax.random.randint(jax.random.fold_in(key, 1), (twos,), 0, 1 << 20) % (room + 1)
    sizes = sizes.at[1:1 + 2 * twos:2].set(donor - passed).at[2:2 + 2 * twos:2].set(taker + passed)
    return sizes[jax.random.permutation(jax.random.fold_in(key, 2), count)]


def centred(stream_key, extent, width, limit, shards=(), held_as=jnp.bfloat16):
    loudness = shard_levels(stream_key, extent, shards, -0.22, 0.18) if shards else 1.0
    values = jax.random.normal(stream_key, extent, jnp.float32) * width * loudness
    return jnp.minimum(jnp.maximum(values, -limit), limit).astype(held_as)


def heavy_noise(own_key, dims, deviation, most, cuts, heavy, kind=jnp.bfloat16):
    array = deviation * jax.random.normal(own_key, dims, jnp.float32)
    if cuts:
        array = array * shard_levels(own_key, dims, cuts, -0.22, 0.18)
    return jnp.clip(with_spikes(array, jax.random.fold_in(own_key, 3), *heavy), -most, most).astype(kind)


def setup_inputs(seed: int = 0) -> dict:
    seeds = jax.random.split(jax.random.key(seed), 6)
    return {
        "queries": draw_queries(jax.random.fold_in(seeds[5], 71), 0),
        "keys": draw_keys(jax.random.fold_in(seeds[5], 71), 0),
        "values": centred(seeds[2], (TOKENS, KVH, HD), 1.0, 6.0, ((0, 16), (1, 2))),
        "out_weight": heavy_noise(seeds[3], (H * HD, D), (H * HD) ** -0.5, 0.125, ((0, 2), (1, 16)), (0, 1, 16, 2.0)),
        "doc_lengths": uneven_parts(seeds[4], NDOCS, TOKENS, REACH * TOK_DEV, 2).astype(jnp.int32),
    }


def doc_index(positions, doc_lengths):
    doc_ends = jnp.cumsum(doc_lengths)
    return jnp.sum((doc_ends[None, :] <= positions[:, None]).astype(jnp.int32), axis=1)


def reference(queries, keys, values, out_weight, doc_lengths):
    block_rows = TOK_DEV
    window = REACH * TOK_DEV
    group_size = H // KVH
    score_scale = 1.0 / (HD ** 0.5)
    positions = jnp.arange(TOKENS, dtype=jnp.int32)
    docs = doc_index(positions, doc_lengths)
    key_padded = jnp.concatenate([jnp.zeros((window, KVH, HD), jnp.bfloat16), keys], axis=0)
    value_padded = jnp.concatenate([jnp.zeros((window, KVH, HD), jnp.bfloat16), values], axis=0)
    doc_padded = jnp.concatenate([jnp.full((window,), -1, jnp.int32), docs], axis=0)

    def one_block(block_index):
        first_row = (block_index * block_rows).astype(jnp.int32)
        query_rows = lax.dynamic_slice_in_dim(queries, first_row, block_rows, 0)
        query_rows = query_rows.reshape(block_rows, KVH, group_size, HD).astype(jnp.float32)
        key_rows = lax.dynamic_slice_in_dim(key_padded, first_row, window + block_rows, 0).astype(jnp.float32)
        value_rows = lax.dynamic_slice_in_dim(value_padded, first_row, window + block_rows, 0).astype(jnp.float32)
        key_doc = lax.dynamic_slice_in_dim(doc_padded, first_row, window + block_rows, 0)
        query_doc = lax.dynamic_slice_in_dim(docs, first_row, block_rows, 0)
        key_pos = first_row - window + jnp.arange(window + block_rows, dtype=jnp.int32)
        query_pos = first_row + jnp.arange(block_rows, dtype=jnp.int32)
        allowed = (key_pos[None, :] >= 0) & (key_pos[None, :] <= query_pos[:, None]) & (key_doc[None, :] == query_doc[:, None])
        scores = jnp.einsum("qgrd,kgd->grqk", query_rows, key_rows) * score_scale
        scores = jnp.where(allowed, scores, -1e30)
        row_max = jnp.max(scores, axis=3)
        expo = jnp.where(allowed, jnp.exp(scores - row_max[..., None]), 0.0)
        row_total = jnp.sum(expo, axis=3)
        rounded = lax.optimization_barrier(expo.astype(jnp.bfloat16))
        output = jnp.einsum("grqk,kgd->grqd", rounded.astype(jnp.float32), value_rows) / row_total[..., None]
        return jnp.transpose(output, (2, 0, 1, 3)).reshape(block_rows, H * HD).astype(jnp.bfloat16)

    attended = lax.map(one_block, jnp.arange(TOKENS // TOK_DEV, dtype=jnp.int32)).reshape(TOKENS, H * HD)
    group_rows = H * HD // N_HEAD
    summed = jnp.zeros((TOKENS, D), jnp.float32)
    for group_index in range(N_HEAD):
        partial_value = jnp.dot(attended[:, group_index * group_rows:(group_index + 1) * group_rows],
                          out_weight[group_index * group_rows:(group_index + 1) * group_rows],
                          preferred_element_type=jnp.float32).astype(jnp.bfloat16)
        partial_value = lax.optimization_barrier(partial_value)
        summed = summed + partial_value.astype(jnp.float32)
    return summed.astype(jnp.bfloat16)
```

```python
import functools
import math

import jax
import jax.numpy as jnp
from jax import lax
from jax.experimental import pallas as pl
from jax.experimental.pallas import tpu as pltpu
from jax.sharding import PartitionSpec as P

MESH = pl.DeviceIdType.MESH


def kernel(
    shape,
    q_in, k_in, v_in, w_ref, lo_ref, out_ref,
    q_ref, k_ref, v_ref,
    q_all, k_all, v_all, w_all, a_all, acc, row_max, row_total, partial, peer, summed, result,
    q_send, q_recv, k_send, k_recv, v_send, v_recv, kz_send, kz_recv, vz_send, vz_recv,
    up_send, up_recv, down_send, down_recv, a_send, a_recv, p_send, p_recv, c_send, c_recv, local_sem,
):
    inner, outer, heads, group, back, span, last = shape
    tok, width = k_in.shape[0], k_in.shape[2]
    part_rows = group * width
    share = outer // heads
    seq, head = lax.axis_index("seq"), lax.axis_index("head")
    o, i = seq // inner, seq % inner

    def remote(src, dst, send, recv, device):
        return pltpu.make_async_remote_copy(
            src_ref=src, dst_ref=dst, send_sem=send, recv_sem=recv, device_id=device, device_id_type=MESH
        )

    def mate(d):
        return (i + d) % inner

    def plane(d):
        return {"seq": o * inner + mate(d)}

    above, below = {"seq": jnp.minimum(seq + inner, outer * inner - 1)}, {"seq": jnp.maximum(seq - inner, 0)}
    has_above, has_below = o + 1 < outer, o >= 1

    barrier = pltpu.get_barrier_semaphore()
    for d in range(1, inner):
        pl.semaphore_signal(barrier, inc=1, device_id=plane(d), device_id_type=MESH)
    for d in range(1, heads):
        pl.semaphore_signal(barrier, inc=1, device_id={"head": (head + d) % heads}, device_id_type=MESH)

    @pl.when(has_above)
    def _():
        pl.semaphore_signal(barrier, inc=1, device_id=above, device_id_type=MESH)

    @pl.when(has_below)
    def _():
        pl.semaphore_signal(barrier, inc=1, device_id=below, device_id_type=MESH)

    pl.semaphore_wait(
        barrier, inner - 1 + heads - 1 + has_above.astype(jnp.int32) + has_below.astype(jnp.int32)
    )

    def kv_copies(d):
        return (
            remote(k_ref.at[mate(d)], k_all.at[0, i], k_send.at[d], k_recv.at[d], plane(d)),
            remote(v_ref.at[mate(d)], v_all.at[0, i], v_send.at[d], v_recv.at[d], plane(d)),
        )

    def q_copy(d):
        return remote(q_ref.at[mate(d)], q_all.at[i], q_send.at[d], q_recv.at[d], plane(d))

    def up_copy(t, first):
        return remote(
            w_ref if first else w_all.at[jnp.maximum(o - t + 1, 0)],
            w_all.at[jnp.maximum(o - t + 1, 0)], up_send.at[t], up_recv.at[t], above,
        )

    def down_copy(t, first):
        return remote(
            w_ref if first else w_all.at[jnp.minimum(o + t - 1, outer - 1)],
            w_all.at[jnp.minimum(o + t - 1, outer - 1)], down_send.at[t], down_recv.at[t], below,
        )

    def got_up(t):
        @pl.when(o >= t)
        def _():
            slot = w_all.at[jnp.maximum(o - t, 0)]
            remote(slot, slot, up_send.at[t], up_recv.at[t], below).wait_recv()

    def got_down(t):
        @pl.when(o + t < outer)
        def _():
            slot = w_all.at[jnp.minimum(o + t, outer - 1)]
            remote(slot, slot, down_send.at[t], down_recv.at[t], above).wait_recv()

    def go_up(t, first=False):
        @pl.when(has_above & (o >= t - 1))
        def _():
            up_copy(t, first).start()

    def go_down(t, first=False):
        @pl.when(has_below & (o + t - 1 < outer))
        def _():
            down_copy(t, first).start()

    if outer > 1:
        go_up(1, True)
        go_down(1, True)
    k_ref[...] = jnp.swapaxes(k_in[...], 0, 1)
    by_head = jnp.swapaxes(v_in[...], 0, 1)
    for j in range(inner):
        v_ref[j] = by_head[j].T
    by_head = jnp.swapaxes(q_in[...], 0, 1)
    for j in range(inner * group):
        q_ref[j // group, :, (j % group) * tok : (j % group + 1) * tok] = by_head[j].T
    for d in range(1, inner):
        for copy in kv_copies(d):
            copy.start()
    for d in range(1, inner):
        q_copy(d).start()

    locals_ = [
        pltpu.make_async_copy(q_ref.at[i], q_all.at[i], local_sem.at[0]),
        pltpu.make_async_copy(k_ref.at[i], k_all.at[0, i], local_sem.at[1]),
        pltpu.make_async_copy(v_ref.at[i], v_all.at[0, i], local_sem.at[2]),
        pltpu.make_async_copy(w_ref, w_all.at[o], local_sem.at[3]),
    ]
    for copy in locals_:
        copy.start()
    for copy in locals_:
        copy.wait()

    def from_mate(d):
        return (i + inner - d) % inner

    for d in range(1, inner):
        k_slot, v_slot = k_all.at[0, from_mate(d)], v_all.at[0, from_mate(d)]
        remote(k_slot, k_slot, k_send.at[d], k_recv.at[d], plane(d)).wait_recv()
        remote(v_slot, v_slot, v_send.at[d], v_recv.at[d], plane(d)).wait_recv()

    def slot_of(ref, b, only_last):
        return ref.at[b, pl.ds(inner - last, last)] if only_last else ref.at[b]

    def lift(b, only_last):
        return (
            remote(slot_of(k_all, b, only_last), slot_of(k_all, b + 1, only_last), kz_send.at[b], kz_recv.at[b + 1], above),
            remote(slot_of(v_all, b, only_last), slot_of(v_all, b + 1, only_last), vz_send.at[b], vz_recv.at[b + 1], above),
        )

    def start_lift(b, only_last):
        @pl.when(has_above & (o >= b))
        def _():
            for copy in lift(b, only_last):
                copy.start()

    def got_lift(b, only_last):
        k_slot, v_slot = slot_of(k_all, b, only_last), slot_of(v_all, b, only_last)
        remote(k_slot, k_slot, kz_send.at[b], kz_recv.at[b], below).wait_recv()
        remote(v_slot, v_slot, vz_send.at[b], vz_recv.at[b], below).wait_recv()

    if back >= 1:
        start_lift(0, back == 1)
    row_max[...] = jnp.full(row_max.shape, -1e30, jnp.float32)
    row_total[...] = jnp.zeros(row_total.shape, jnp.float32)
    acc[...] = jnp.zeros(acc.shape, jnp.float32)
    factor = math.log2(math.e) / math.sqrt(width)

    def tile(b, qb, kb, diagonal):
        key_pos = ((o - b) * inner + kb) * tok + lax.broadcasted_iota(jnp.int32, (tok, tok), 0)
        allowed = key_pos >= lo_ref[qb]
        if diagonal:
            allowed &= lax.broadcasted_iota(jnp.int32, (tok, tok), 0) <= lax.broadcasted_iota(
                jnp.int32, (tok, tok), 1
            )
        keys_here, values_here = k_all[b, kb], v_all[b, kb]
        for r in range(group):
            cols = pl.ds(r * tok, tok)
            scores = jnp.dot(keys_here, q_all[qb, :, cols], preferred_element_type=jnp.float32)
            scores = jnp.where(allowed, scores * factor, -1e30)
            old_max = row_max[qb, :, cols]
            new_max = jnp.maximum(old_max, jnp.max(scores, axis=0, keepdims=True))
            weights = jnp.exp2(scores - new_max)
            rescale = jnp.exp2(old_max - new_max)
            row_max[qb, :, cols] = new_max
            row_total[qb, :, cols] = row_total[qb, :, cols] * rescale + jnp.sum(weights, axis=0, keepdims=True)
            acc[qb, :, cols] = acc[qb, :, cols] * rescale + jnp.dot(
                values_here, weights.astype(jnp.bfloat16), preferred_element_type=jnp.float32
            )

    def own_rows(qb, carry):
        tile(0, qb, qb, True)

        def own_keys(kb, inside):
            tile(0, qb, kb, False)
            return inside

        return lax.fori_loop(0, qb, own_keys, carry)

    own_rows(i, 0)
    for d in range(1, inner):
        q_slot = q_all.at[from_mate(d)]
        remote(q_slot, q_slot, q_send.at[d], q_recv.at[d], plane(d)).wait_recv()
        own_rows(from_mate(d), 0)

    def attend(b, qb):
        def cols(kb, inside):
            tile(b, qb, kb, False)
            return inside

        lax.fori_loop(jnp.maximum(b * inner + qb - span, 0), inner, cols, 0)

    def middle(b):
        @pl.when(o >= b)
        def _():
            got_lift(b, False)

        @pl.when(has_above & (o >= b))
        def _():
            for copy in lift(b, False):
                copy.start()

    if outer > 1:
        got_down(1)
    if outer > 2:
        go_down(2)
    def whole_slot(b, carry):
        middle(b)
        return carry

    if back > 2:
        middle(1)
    elif back == 2:
        @pl.when(o >= 1)
        def _():
            got_lift(1, False)

        start_lift(1, True)
    elif back == 1:
        @pl.when(o >= 1)
        def _():
            got_lift(1, True)
    early = inner // 2 if back > 1 else 0

    def early_rows(qb, carry):
        attend(1, qb)
        return carry

    if early:
        @pl.when(o >= 1)
        def _():
            lax.fori_loop(inner - early, inner, early_rows, 0)

    if back > 2:
        lax.fori_loop(2, back - 1, whole_slot, 0)

        @pl.when(o >= back - 1)
        def _():
            got_lift(back - 1, False)

        start_lift(back - 1, True)
    if outer > 1:
        got_up(1)
    if outer > 2:
        go_up(2)

    def a_copy(qb, d):
        slot = a_all.at[qb, i]
        return remote(slot, slot, a_send.at[qb, d], a_recv.at[qb, d], plane(d))

    def send_rows(qb):
        for d in range(1, inner):
            a_copy(qb, d).start()

    def finish(qb):
        for r in range(group):
            cols = pl.ds(r * tok, tok)
            normal = acc[qb, :, cols] / row_total[qb, :, cols]
            a_all[qb, i, :, r * width : (r + 1) * width] = normal.T.astype(jnp.bfloat16)

    deepest = min(inner, span + inner - back * inner)

    def finish_rows(k, carry):
        qb = inner - 1 - k

        def slots(b, inside):
            attend(b, qb)
            return inside

        lax.fori_loop(jnp.where(k < early, 2, 1), jnp.minimum(o, back - 1) + 1, slots, 0)
        if back > 1:
            @pl.when((o >= back) & (qb == deepest - 1))
            def _():
                got_lift(back, True)

        if back >= 1:
            @pl.when((o >= back) & (qb < deepest))
            def _():
                attend(back, qb)

        finish(qb)
        send_rows(qb)
        return carry

    lax.fori_loop(0, inner, finish_rows, 0)

    def hop(t, carry):
        got_down(t - 1)
        go_down(t)
        got_up(t - 1)
        go_up(t)
        return carry

    if outer > 3:
        got_down(2)
        go_down(3)
        got_up(2)
        go_up(3)
        lax.fori_loop(4, outer, hop, 0)
    def multiply(qb, s):
        value = jnp.dot(a_all[qb, 0], w_all[s, 0:part_rows, :], preferred_element_type=jnp.float32)
        for j in range(1, inner):
            value += jnp.dot(
                a_all[qb, j], w_all[s, j * part_rows : (j + 1) * part_rows, :], preferred_element_type=jnp.float32
            )
        partial[s, qb] = value.astype(jnp.bfloat16)

    def p_copy(s):
        to = s // share
        d = (to + heads - head) % heads
        return remote(
            partial.at[s], peer.at[d, s % share], p_send.at[s], p_recv.at[d, s % share], {"head": to}
        )

    def give(s):
        @pl.when(s // share != head)
        def _():
            p_copy(s).start()

    def c_copy(sl, d):
        return remote(summed.at[sl, mate(d)], result.at[sl, i], c_send.at[sl, d], c_recv.at[sl, d], plane(d))

    def absorb(s):
        @pl.when(s // share == head)
        def _():
            sl = s % share
            for d in range(1, heads):
                slot = peer.at[d, sl]
                remote(slot, slot, p_send.at[s], p_recv.at[d, sl], {"head": (head + d) % heads}).wait_recv()

            def rows(j, carry):
                total = partial[s, j].astype(jnp.float32)
                for d in range(1, heads):
                    total = total + peer[d, sl, j].astype(jnp.float32)
                summed[sl, j] = total.astype(jnp.bfloat16)
                return carry

            lax.fori_loop(0, inner, rows, 0)
            for d in range(1, inner):
                c_copy(sl, d).start()
            result[sl, i] = summed[sl, i]

    def near(t, act):
        @pl.when(o - t >= 0)
        def _():
            act(jnp.maximum(o - t, 0))

        @pl.when((o + t < outer) & (t > 0))
        def _():
            act(jnp.minimum(o + t, outer - 1))

    near_count = max(outer - 1, 1)

    def got_rows(qb):
        for d in range(1, inner):
            slot = a_all.at[qb, from_mate(d)]
            remote(slot, slot, a_send.at[qb, d], a_recv.at[qb, d], plane(d)).wait_recv()

    def early_blocks(k, carry):
        qb = inner - 1 - k
        got_rows(qb)

        def shards(t, inside):
            near(t, lambda s: multiply(qb, s))
            return inside

        lax.fori_loop(0, near_count, shards, 0)
        return carry

    lax.fori_loop(0, inner - 1, early_blocks, 0)
    got_rows(0)

    def final_block(t, carry):
        def act(s):
            multiply(0, s)
            give(s)

        near(t, act)

        @pl.when(t >= 1)
        def _():
            near(t - 1, absorb)

        return carry

    lax.fori_loop(0, near_count, final_block, 0)
    near(near_count - 1, absorb)
    if outer > 1:
        if outer > 2:
            got_down(outer - 1)
            got_up(outer - 1)

        def far(s):
            def rows(qb, carry):
                multiply(qb, s)
                return carry

            lax.fori_loop(0, inner, rows, 0)
            give(s)

        near(outer - 1, far)
        near(outer - 1, absorb)
    for sl in range(share):
        for d in range(1, inner):
            slot = result.at[sl, from_mate(d)]
            remote(slot, slot, c_send.at[sl, d], c_recv.at[sl, d], plane(d)).wait_recv()
    wide = out_ref.shape[1] // (share * inner)
    for s in range(share):
        for j in range(inner):
            out_ref[:, (s * inner + j) * wide : (s * inner + j + 1) * wide] = result[s, j]

    for d in range(1, inner):
        for copy in kv_copies(d):
            copy.wait_send()
        q_copy(d).wait_send()
        for qb in range(inner):
            a_copy(qb, d).wait_send()
        for sl in range(share):
            c_copy(sl, d).wait_send()

    def given(s, carry):
        @pl.when(s // share != head)
        def _():
            p_copy(s).wait_send()

        return carry

    lax.fori_loop(0, outer, given, 0)

    def lift_done(b, only_last):
        @pl.when(has_above & (o >= b))
        def _():
            for copy in lift(b, only_last):
                copy.wait_send()

    if back > 1:
        def lift_sent(b, carry):
            lift_done(b, False)
            return carry

        lax.fori_loop(0, back - 1, lift_sent, 0)
    if back >= 1:
        lift_done(back - 1, True)

    def hop_sent(t, first):
        @pl.when(has_above & (o >= t - 1))
        def _():
            up_copy(t, first).wait_send()

        @pl.when(has_below & (o + t - 1 < outer))
        def _():
            down_copy(t, first).wait_send()

    def later_sent(t, carry):
        hop_sent(t, False)
        return carry

    if outer > 1:
        hop_sent(1, True)
        lax.fori_loop(2, outer, later_sent, 0)


def paired_kernel(
    shape,
    q_in, k_in, v_in, w_ref, lo_ref, out_ref,
    q_ref, k_ref, v_ref,
    q_all, k_all, v_all, w_all, a_all, acc, row_max, row_total, part, peer, first_in, second_in, final, final_in,
    q_send, q_recv, k_send, k_recv, v_send, v_recv, kz_send, kz_recv, vz_send, vz_recv,
    w_send, w_recv, f_send, f_recv, a_send, a_recv, d_send, d_recv,
    r_send, r_recv, s_send, s_recv, o_send, o_recv, local_sem,
):
    inner, outer, heads, group, back, span, last = shape
    tok, width = k_in.shape[0], k_in.shape[2]
    rows = group * width
    wide = w_ref.shape[1]
    half = (inner // 2) * wide
    seq, head = lax.axis_index("seq"), lax.axis_index("head")
    o, i = seq // inner, seq % inner
    ix, iy = i % 2, i // 2
    low, high = o % 2, o // 2
    kept = (head + high) % 2

    def remote(src, dst, send, recv, device):
        return pltpu.make_async_remote_copy(
            src_ref=src, dst_ref=dst, send_sem=send, recv_sem=recv, device_id=device, device_id_type=MESH
        )

    def mate(d):
        return (i + d) % inner

    def from_mate(d):
        return (i + inner - d) % inner

    def plane(d):
        return {"seq": o * inner + mate(d)}

    across = ({"seq": o * inner + iy * 2 + 1 - ix}, {"seq": o * inner + (1 - iy) * 2 + ix})
    pair = {"seq": (o + 1 - 2 * low) * inner + i}
    far = {"seq": ((o + 2) % outer) * inner + i}
    other = {"head": (head + 1) % heads}
    above, below = {"seq": jnp.minimum(seq + inner, outer * inner - 1)}, {"seq": jnp.maximum(seq - inner, 0)}
    has_above, has_below = o + 1 < outer, o >= 1

    barrier = pltpu.get_barrier_semaphore()
    for d in range(1, inner):
        pl.semaphore_signal(barrier, inc=1, device_id=plane(d), device_id_type=MESH)
    pl.semaphore_signal(barrier, inc=1, device_id=other, device_id_type=MESH)
    pl.semaphore_signal(barrier, inc=1, device_id=far, device_id_type=MESH)

    @pl.when(has_above)
    def _():
        pl.semaphore_signal(barrier, inc=1, device_id=above, device_id_type=MESH)

    @pl.when(has_below)
    def _():
        pl.semaphore_signal(barrier, inc=1, device_id=below, device_id_type=MESH)

    pl.semaphore_wait(barrier, inner + 1 + has_above.astype(jnp.int32) + has_below.astype(jnp.int32))

    def kv_copies(d):
        return (
            remote(k_ref.at[mate(d)], k_all.at[0, i], k_send.at[d], k_recv.at[d], plane(d)),
            remote(v_ref.at[mate(d)], v_all.at[0, i], v_send.at[d], v_recv.at[d], plane(d)),
        )

    def q_copy(d):
        return remote(q_ref.at[mate(d)], q_all.at[i], q_send.at[d], q_recv.at[d], plane(d))

    def w_rows(j):
        return w_ref.at[pl.ds(pl.multiple_of(j * rows, rows), rows)]

    def w_copy(d):
        return remote(w_rows(mate(d)), w_all.at[0, i], w_send.at[d], w_recv.at[d], plane(d))

    def far_copy(d):
        src = w_rows(i) if d == 0 else w_all.at[0, from_mate(d)]
        return remote(src, w_all.at[1, from_mate(d)], f_send.at[d], f_recv.at[d], far)

    far_copy(0).start()
    k_ref[...] = jnp.swapaxes(k_in[...], 0, 1)
    for d in range(1, inner):
        kv_copies(d)[0].start()
    by_head = jnp.swapaxes(v_in[...], 0, 1)
    for j in range(inner):
        v_ref[j] = by_head[j].T
    for d in range(1, inner):
        kv_copies(d)[1].start()
    by_head = jnp.swapaxes(q_in[...], 0, 1)
    for j in range(inner * group):
        q_ref[j // group, :, (j % group) * tok : (j % group + 1) * tok] = by_head[j].T
    for d in range(1, inner):
        q_copy(d).start()
    for d in range(1, inner):
        w_copy(d).start()

    locals_ = [
        pltpu.make_async_copy(q_ref.at[i], q_all.at[i], local_sem.at[0]),
        pltpu.make_async_copy(k_ref.at[i], k_all.at[0, i], local_sem.at[1]),
        pltpu.make_async_copy(v_ref.at[i], v_all.at[0, i], local_sem.at[2]),
        pltpu.make_async_copy(w_rows(i), w_all.at[0, i], local_sem.at[3]),
    ]
    for copy in locals_:
        copy.start()
    row_max[...] = jnp.full(row_max.shape, -1e30, jnp.float32)
    row_total[...] = jnp.zeros(row_total.shape, jnp.float32)
    acc[...] = jnp.zeros(acc.shape, jnp.float32)
    for copy in locals_:
        copy.wait()

    for d in range(1, inner):
        k_slot, v_slot = k_all.at[0, from_mate(d)], v_all.at[0, from_mate(d)]
        remote(k_slot, k_slot, k_send.at[d], k_recv.at[d], plane(d)).wait_recv()
        remote(v_slot, v_slot, v_send.at[d], v_recv.at[d], plane(d)).wait_recv()

    def slot_of(ref, b, only_last):
        return ref.at[b, pl.ds(inner - last, last)] if only_last else ref.at[b]

    def lift(b):
        only_last = b == back - 1
        return (
            remote(slot_of(k_all, b, only_last), slot_of(k_all, b + 1, only_last), kz_send.at[b], kz_recv.at[b + 1], above),
            remote(slot_of(v_all, b, only_last), slot_of(v_all, b + 1, only_last), vz_send.at[b], vz_recv.at[b + 1], above),
        )

    def start_lift(b):
        @pl.when(has_above & (o >= b))
        def _():
            for copy in lift(b):
                copy.start()

    def got_lift(b):
        @pl.when(o >= b)
        def _():
            k_slot, v_slot = slot_of(k_all, b, b == back), slot_of(v_all, b, b == back)
            remote(k_slot, k_slot, kz_send.at[b], kz_recv.at[b], below).wait_recv()
            remote(v_slot, v_slot, vz_send.at[b], vz_recv.at[b], below).wait_recv()

    if back >= 1:
        start_lift(0)
    factor = math.log2(math.e) / math.sqrt(width)

    def tile(b, qb, kb, diagonal):
        key_pos = ((o - b) * inner + kb) * tok + lax.broadcasted_iota(jnp.int32, (tok, tok), 0)
        allowed = key_pos >= lo_ref[qb]
        if diagonal:
            allowed &= lax.broadcasted_iota(jnp.int32, (tok, tok), 0) <= lax.broadcasted_iota(
                jnp.int32, (tok, tok), 1
            )
        keys_here, values_here = k_all[b, kb], v_all[b, kb]
        raw = [
            jnp.dot(keys_here, q_all[qb, :, r * tok : (r + 1) * tok], preferred_element_type=jnp.float32)
            for r in range(group)
        ]
        for r in range(group):
            cols = pl.ds(r * tok, tok)
            scores = jnp.where(allowed, raw[r] * factor, -1e30)
            old_max = row_max[qb, :, cols]
            new_max = jnp.maximum(old_max, jnp.max(scores, axis=0, keepdims=True))
            weights = jnp.exp2(scores - new_max)
            rescale = jnp.exp2(old_max - new_max)
            row_max[qb, :, cols] = new_max
            row_total[qb, :, cols] = row_total[qb, :, cols] * rescale + jnp.sum(weights, axis=0, keepdims=True)
            acc[qb, :, cols] = acc[qb, :, cols] * rescale + jnp.dot(
                values_here, weights.astype(jnp.bfloat16), preferred_element_type=jnp.float32
            )

    def own_rows(qb):
        tile(0, qb, qb, True)

        def own_keys(kb, inside):
            tile(0, qb, kb, False)
            return inside

        lax.fori_loop(0, qb, own_keys, 0)

    def attend(b, qb):
        def cols(kb, inside):
            tile(b, qb, kb, False)
            return inside

        lax.fori_loop(jnp.maximum(b * inner + qb - span, 0), inner, cols, 0)

    def own_from(d, carry):
        @pl.when(d >= 1)
        def _():
            q_slot = q_all.at[from_mate(d)]
            remote(q_slot, q_slot, q_send.at[d], q_recv.at[d], plane(d)).wait_recv()

        own_rows(from_mate(d))
        return carry

    lax.fori_loop(0, inner, own_from, 0)

    def rows_of(b, begin, end):
        def one(k, carry):
            attend(b, inner - 1 - k)
            return carry

        @pl.when(o >= b)
        def _():
            lax.fori_loop(begin, end, one, 0)

    if back > 1:
        got_lift(1)
        start_lift(1)
        rows_of(1, 0, inner // 2)
    for d in range(1, inner):
        slot = w_all.at[0, from_mate(d)]
        remote(slot, slot, w_send.at[d], w_recv.at[d], plane(d)).wait_recv()
        far_copy(d).start()
    if back > 1:
        rows_of(1, inner // 2, inner)
    for b in range(2, back):
        got_lift(b)
        start_lift(b)
        if b < back - 1:
            rows_of(b, 0, inner)

    def a_copy(qb):
        return remote(a_all.at[0, qb], a_all.at[1, qb], a_send.at[qb], a_recv.at[qb], pair)

    def finish(qb):
        for r in range(group):
            cols = pl.ds(r * tok, tok)
            normal = acc[qb, :, cols] / row_total[qb, :, cols]
            a_all[0, qb, :, r * width : (r + 1) * width] = normal.T.astype(jnp.bfloat16)

    def give(qb, side):
        return remote(part.at[side, qb], peer.at[qb], d_send.at[qb], d_recv.at[qb], other)

    def multiply(side, qb):
        if side == 0:
            slot = a_all.at[1, qb]
            remote(slot, slot, a_send.at[qb], a_recv.at[qb], pair).wait_recv()
        for p in range(2):
            for m in range(inner):
                value = jnp.dot(a_all[p, qb], w_all[side, m], preferred_element_type=jnp.float32)
                c, mm = m // 2, m % 2
                part[side, qb, c, p, :, mm * wide : (mm + 1) * wide] = value.astype(jnp.bfloat16)

        @pl.when(kept != side)
        def _():
            give(qb, side).start()

    def first_copy(qb, c):
        t = (qb // 2) if c == 0 else (qb % 2)
        return remote(part.at[kept, qb, c], first_in.at[c, t], r_send.at[c, t], r_recv.at[c, t], across[c])

    def is_sent(qb, c):
        return (qb % 2 != ix) if c == 0 else (qb // 2 != iy)

    def combine(qb):
        slot = peer.at[qb]
        remote(slot, slot, d_send.at[qb], d_recv.at[qb], other).wait_recv()
        for c in range(2):
            total = part[kept, qb, c].astype(jnp.float32) + peer[qb, c].astype(jnp.float32)
            part[kept, qb, c] = total.astype(jnp.bfloat16)

            @pl.when(is_sent(qb, c))
            def _():
                first_copy(qb, c).start()

    def kept_block(c, t):
        return 2 * t + ix if c == 0 else 2 * iy + t

    def second_copy(c, t):
        return remote(part.at[kept, kept_block(c, t), c], second_in.at[c], s_send.at[c], s_recv.at[c], across[1 - c])

    def first_sum(c, t):
        slot = first_in.at[c, t]
        remote(slot, slot, r_send.at[c, t], r_recv.at[c, t], across[c]).wait_recv()
        qb = kept_block(c, t)
        total = part[kept, qb, c].astype(jnp.float32) + first_in[c, t].astype(jnp.float32)
        part[kept, qb, c] = total.astype(jnp.bfloat16)

        @pl.when(t != (iy if c == 0 else ix))
        def _():
            second_copy(c, t).start()

    def first_sums():
        for t in (1, 0):
            for c in range(2):
                first_sum(c, t)

    def out_copy(c):
        return remote(final.at[c], final_in.at[c], o_send.at[c], o_recv.at[c], pair)

    def columns(parity, c):
        return pl.ds(pl.multiple_of(parity * (2 * half) + c * half, half), half)

    def second_sum(c):
        slot = second_in.at[c]
        remote(slot, slot, s_send.at[c], s_recv.at[c], across[1 - c]).wait_recv()
        total = part[kept, i, c].astype(jnp.float32) + second_in[c].astype(jnp.float32)
        total = total.astype(jnp.bfloat16)
        final[c] = total[1]
        out_copy(c).start()
        out_ref[:, columns(low, c)] = total[0]

    deepest = min(inner, span + inner - back * inner)

    def finish_rows(k, carry):
        qb = inner - 1 - k

        @pl.when(o >= back - 1)
        def _():
            if back > 2:
                attend(back - 1, qb)

        @pl.when((o >= back) & (qb == deepest - 1))
        def _():
            got_lift(back)

        @pl.when((o >= back) & (qb < deepest))
        def _():
            attend(back, qb)

        finish(qb)
        a_copy(qb).start()

        @pl.when(k >= 1)
        def _():
            multiply(0, qb + 1)

        @pl.when((k >= 2) & (kept == 0))
        def _():
            combine(qb + 2)

        return carry

    lax.fori_loop(0, inner, finish_rows, 0)
    multiply(0, 0)

    @pl.when(kept == 0)
    def _():
        combine(1)
        combine(0)
        first_sums()

    for d in range(inner):
        slot = w_all.at[1, from_mate(d)]
        remote(slot, slot, f_send.at[d], f_recv.at[d], far).wait_recv()

    def far_rows(k, carry):
        qb = inner - 1 - k

        @pl.when(k < inner)
        def _():
            multiply(1, qb)

        @pl.when((k >= 1) & (kept == 1))
        def _():
            combine(qb + 1)

        return carry

    lax.fori_loop(0, inner + 1, far_rows, 0)

    @pl.when(kept == 1)
    def _():
        first_sums()

    for c in range(2):
        second_sum(c)
    for c in range(2):
        slot = final_in.at[c]
        remote(slot, slot, o_send.at[c], o_recv.at[c], pair).wait_recv()
        out_ref[:, columns(1 - low, c)] = final_in[c]

    for d in range(1, inner):
        for copy in kv_copies(d):
            copy.wait_send()
        q_copy(d).wait_send()
        w_copy(d).wait_send()
    for d in range(inner):
        far_copy(d).wait_send()
    for b in range(back):
        @pl.when(has_above & (o >= b))
        def _():
            for copy in lift(b):
                copy.wait_send()
    for qb in range(inner):
        a_copy(qb).wait_send()
        give(qb, 1 - kept).wait_send()
        for c in range(2):
            @pl.when(is_sent(qb, c))
            def _():
                first_copy(qb, c).wait_send()
    for c in range(2):
        second_copy(c, 1 - (iy if c == 0 else ix)).wait_send()
        out_copy(c).wait_send()


def paired_scratch(inner, heads, group, back, tok, width, wide):
    bf16, f32 = jnp.bfloat16, jnp.float32
    dma = pltpu.SemaphoreType.DMA
    half = (inner // 2) * wide
    scratch = [
        pltpu.VMEM((inner, width, group * tok), bf16),
        pltpu.VMEM((inner, tok, width), bf16),
        pltpu.VMEM((inner, width, tok), bf16),
        pltpu.VMEM((inner, width, group * tok), bf16),
        pltpu.VMEM((back + 1, inner, tok, width), bf16),
        pltpu.VMEM((back + 1, inner, width, tok), bf16),
        pltpu.VMEM((2, inner, group * width, wide), bf16),
        pltpu.VMEM((2, inner, tok, group * width), bf16),
        pltpu.VMEM((inner, width, group * tok), f32),
        pltpu.VMEM((inner, 1, group * tok), f32),
        pltpu.VMEM((inner, 1, group * tok), f32),
        pltpu.VMEM((2, inner, 2, 2, tok, half), bf16),
        pltpu.VMEM((inner, 2, 2, tok, half), bf16),
        pltpu.VMEM((2, 2, 2, tok, half), bf16),
        pltpu.VMEM((2, 2, tok, half), bf16),
        pltpu.VMEM((2, tok, half), bf16),
        pltpu.VMEM((2, tok, half), bf16),
    ]
    scratch += [dma((inner,))] * 6 + [dma((back + 1,))] * 4 + [dma((inner,))] * 8
    return scratch + [dma((2, 2))] * 2 + [dma((2,))] * 4 + [dma((4,))]


def body(queries, keys, values, out_weight, doc_lengths):
    tok, heads_here, width = queries.shape
    inner = keys.shape[1]
    group = heads_here // inner
    count = lax.axis_size("seq")
    heads = lax.axis_size("head")
    outer = count // inner
    span = count // 2 + 1
    plane_rows = inner * tok
    reach = span * tok - 1
    back = min(outer - 1, -(-reach // plane_rows))
    last = min(inner, -(-(reach - (back - 1) * plane_rows) // tok))
    share = outer // heads
    depth, wide = out_weight.shape

    positions = (lax.axis_index("seq") // inner) * plane_rows + jnp.arange(plane_rows, dtype=jnp.int32)
    ends = jnp.cumsum(doc_lengths)
    starts = jnp.max(jnp.where(ends[None, :] <= positions[:, None], ends[None, :], 0), axis=1)
    starts = starts.reshape(inner, 1, tok)

    bf16, f32 = jnp.bfloat16, jnp.float32
    dma = pltpu.SemaphoreType.DMA
    scratch = [
        pltpu.VMEM((inner, width, group * tok), bf16),
        pltpu.VMEM((inner, tok, width), bf16),
        pltpu.VMEM((inner, width, tok), bf16),
        pltpu.VMEM((inner, width, group * tok), bf16),
        pltpu.VMEM((back + 1, inner, tok, width), bf16),
        pltpu.VMEM((back + 1, inner, width, tok), bf16),
        pltpu.VMEM((outer, depth, wide), bf16),
        pltpu.VMEM((inner, inner, tok, group * width), bf16),
        pltpu.VMEM((inner, width, group * tok), f32),
        pltpu.VMEM((inner, 1, group * tok), f32),
        pltpu.VMEM((inner, 1, group * tok), f32),
        pltpu.VMEM((outer, inner, tok, wide), bf16),
        pltpu.VMEM((heads, share, inner, tok, wide), bf16),
        pltpu.VMEM((share, inner, tok, wide), bf16),
        pltpu.VMEM((share, inner, tok, wide), bf16),
    ]
    scratch += [dma((inner,))] * 6 + [dma((back + 1,))] * 4 + [dma((outer,))] * 4
    scratch += [dma((inner, inner))] * 2 + [dma((outer,)), dma((heads, share))] + [dma((share, inner))] * 2 + [dma((4,))]
    shape = (inner, outer, heads, group, back, span, last)
    run = kernel
    if inner == 4 and outer == 4 and heads == 2 and back > 2:
        run, scratch = paired_kernel, paired_scratch(inner, heads, group, back, tok, width, wide)
    return pl.pallas_call(
        functools.partial(run, shape),
        out_shape=jax.ShapeDtypeStruct((tok, share * inner * wide), bf16),
        in_specs=[pl.BlockSpec(memory_space=pltpu.VMEM)] * 5,
        out_specs=pl.BlockSpec(memory_space=pltpu.VMEM),
        scratch_shapes=scratch,
        compiler_params=pltpu.CompilerParams(
            collective_id=0, has_side_effects=True, vmem_limit_bytes=60 * 1024 * 1024
        ),
    )(queries, keys, values, out_weight, starts)


def solution(mesh):
    placed = (
        P("seq", "head", None),
        P("seq", "head", None),
        P("seq", "head", None),
        P("head", "seq"),
        P(),
    )
    return jax.shard_map(
        body, mesh=mesh, in_specs=placed, out_specs=P("seq", "head"), check_vma=False
    )
```

```python
import functools
import math

import jax
import jax.numpy as jnp
from jax import lax
from jax.experimental import pallas as pl
from jax.experimental.pallas import tpu as pltpu
from jax.sharding import PartitionSpec as P

MESH = pl.DeviceIdType.MESH


def kernel(
    shape,
    q_in, k_in, v_in, w_ref, lo_ref, out_ref,
    q_ref, k_ref, v_ref,
    q_all, k_all, v_all, w_all, a_all, acc, row_max, row_total, partial, peer, summed, result,
    q_send, q_recv, k_send, k_recv, v_send, v_recv, kz_send, kz_recv, vz_send, vz_recv,
    up_send, up_recv, down_send, down_recv, a_send, a_recv, p_send, p_recv, c_send, c_recv, local_sem,
):
    inner, outer, heads, group, back, span, last = shape
    tok, width = k_in.shape[0], k_in.shape[2]
    part_rows = group * width
    share = outer // heads
    seq, head = lax.axis_index("seq"), lax.axis_index("head")
    o, i = seq // inner, seq % inner

    def remote(src, dst, send, recv, device):
        return pltpu.make_async_remote_copy(
            src_ref=src, dst_ref=dst, send_sem=send, recv_sem=recv, device_id=device, device_id_type=MESH
        )

    def mate(d):
        return (i + d) % inner

    def plane(d):
        return {"seq": o * inner + mate(d)}

    above, below = {"seq": jnp.minimum(seq + inner, outer * inner - 1)}, {"seq": jnp.maximum(seq - inner, 0)}
    has_above, has_below = o + 1 < outer, o >= 1

    barrier = pltpu.get_barrier_semaphore()
    for d in range(1, inner):
        pl.semaphore_signal(barrier, inc=1, device_id=plane(d), device_id_type=MESH)
    for d in range(1, heads):
        pl.semaphore_signal(barrier, inc=1, device_id={"head": (head + d) % heads}, device_id_type=MESH)

    @pl.when(has_above)
    def _():
        pl.semaphore_signal(barrier, inc=1, device_id=above, device_id_type=MESH)

    @pl.when(has_below)
    def _():
        pl.semaphore_signal(barrier, inc=1, device_id=below, device_id_type=MESH)

    pl.semaphore_wait(
        barrier, inner - 1 + heads - 1 + has_above.astype(jnp.int32) + has_below.astype(jnp.int32)
    )

    def kv_copies(d):
        return (
            remote(k_ref.at[mate(d)], k_all.at[0, i], k_send.at[d], k_recv.at[d], plane(d)),
            remote(v_ref.at[mate(d)], v_all.at[0, i], v_send.at[d], v_recv.at[d], plane(d)),
        )

    def q_copy(d):
        return remote(q_ref.at[mate(d)], q_all.at[i], q_send.at[d], q_recv.at[d], plane(d))

    def up_copy(t, first):
        return remote(
            w_ref if first else w_all.at[jnp.maximum(o - t + 1, 0)],
            w_all.at[jnp.maximum(o - t + 1, 0)], up_send.at[t], up_recv.at[t], above,
        )

    def down_copy(t, first):
        return remote(
            w_ref if first else w_all.at[jnp.minimum(o + t - 1, outer - 1)],
            w_all.at[jnp.minimum(o + t - 1, outer - 1)], down_send.at[t], down_recv.at[t], below,
        )

    def got_up(t):
        @pl.when(o >= t)
        def _():
            slot = w_all.at[jnp.maximum(o - t, 0)]
            remote(slot, slot, up_send.at[t], up_recv.at[t], below).wait_recv()

    def got_down(t):
        @pl.when(o + t < outer)
        def _():
            slot = w_all.at[jnp.minimum(o + t, outer - 1)]
            remote(slot, slot, down_send.at[t], down_recv.at[t], above).wait_recv()

    def go_up(t, first=False):
        @pl.when(has_above & (o >= t - 1))
        def _():
            up_copy(t, first).start()

    def go_down(t, first=False):
        @pl.when(has_below & (o + t - 1 < outer))
        def _():
            down_copy(t, first).start()

    if outer > 1:
        go_up(1, True)
        go_down(1, True)
    k_ref[...] = jnp.swapaxes(k_in[...], 0, 1)
    by_head = jnp.swapaxes(v_in[...], 0, 1)
    for j in range(inner):
        v_ref[j] = by_head[j].T
    by_head = jnp.swapaxes(q_in[...], 0, 1)
    for j in range(inner * group):
        q_ref[j // group, :, (j % group) * tok : (j % group + 1) * tok] = by_head[j].T
    for d in range(1, inner):
        for copy in kv_copies(d):
            copy.start()
    for d in range(1, inner):
        q_copy(d).start()

    locals_ = [
        pltpu.make_async_copy(q_ref.at[i], q_all.at[i], local_sem.at[0]),
        pltpu.make_async_copy(k_ref.at[i], k_all.at[0, i], local_sem.at[1]),
        pltpu.make_async_copy(v_ref.at[i], v_all.at[0, i], local_sem.at[2]),
        pltpu.make_async_copy(w_ref, w_all.at[o], local_sem.at[3]),
    ]
    for copy in locals_:
        copy.start()
    for copy in locals_:
        copy.wait()

    def from_mate(d):
        return (i + inner - d) % inner

    for d in range(1, inner):
        k_slot, v_slot = k_all.at[0, from_mate(d)], v_all.at[0, from_mate(d)]
        remote(k_slot, k_slot, k_send.at[d], k_recv.at[d], plane(d)).wait_recv()
        remote(v_slot, v_slot, v_send.at[d], v_recv.at[d], plane(d)).wait_recv()

    def slot_of(ref, b, only_last):
        return ref.at[b, pl.ds(inner - last, last)] if only_last else ref.at[b]

    def lift(b, only_last):
        return (
            remote(slot_of(k_all, b, only_last), slot_of(k_all, b + 1, only_last), kz_send.at[b], kz_recv.at[b + 1], above),
            remote(slot_of(v_all, b, only_last), slot_of(v_all, b + 1, only_last), vz_send.at[b], vz_recv.at[b + 1], above),
        )

    def start_lift(b, only_last):
        @pl.when(has_above & (o >= b))
        def _():
            for copy in lift(b, only_last):
                copy.start()

    def got_lift(b, only_last):
        k_slot, v_slot = slot_of(k_all, b, only_last), slot_of(v_all, b, only_last)
        remote(k_slot, k_slot, kz_send.at[b], kz_recv.at[b], below).wait_recv()
        remote(v_slot, v_slot, vz_send.at[b], vz_recv.at[b], below).wait_recv()

    if back >= 1:
        start_lift(0, back == 1)
    row_max[...] = jnp.full(row_max.shape, -1e30, jnp.float32)
    row_total[...] = jnp.zeros(row_total.shape, jnp.float32)
    acc[...] = jnp.zeros(acc.shape, jnp.float32)
    factor = math.log2(math.e) / math.sqrt(width)

    def tile(b, qb, kb, diagonal):
        key_pos = ((o - b) * inner + kb) * tok + lax.broadcasted_iota(jnp.int32, (tok, tok), 0)
        allowed = key_pos >= lo_ref[qb]
        if diagonal:
            allowed &= lax.broadcasted_iota(jnp.int32, (tok, tok), 0) <= lax.broadcasted_iota(
                jnp.int32, (tok, tok), 1
            )
        keys_here, values_here = k_all[b, kb], v_all[b, kb]
        raw = [
            jnp.dot(keys_here, q_all[qb, :, r * tok : (r + 1) * tok], preferred_element_type=jnp.float32)
            for r in range(group)
        ]
        for r in range(group):
            cols = pl.ds(r * tok, tok)
            scores = jnp.where(allowed, raw[r] * factor, -1e30)
            old_max = row_max[qb, :, cols]
            new_max = jnp.maximum(old_max, jnp.max(scores, axis=0, keepdims=True))
            weights = jnp.exp2(scores - new_max)
            rescale = jnp.exp2(old_max - new_max)
            row_max[qb, :, cols] = new_max
            row_total[qb, :, cols] = row_total[qb, :, cols] * rescale + jnp.sum(weights, axis=0, keepdims=True)
            acc[qb, :, cols] = acc[qb, :, cols] * rescale + jnp.dot(
                values_here, weights.astype(jnp.bfloat16), preferred_element_type=jnp.float32
            )

    def own_rows(qb, carry):
        tile(0, qb, qb, True)

        def own_keys(kb, inside):
            tile(0, qb, kb, False)
            return inside

        return lax.fori_loop(0, qb, own_keys, carry)

    own_rows(i, 0)
    for d in range(1, inner):
        q_slot = q_all.at[from_mate(d)]
        remote(q_slot, q_slot, q_send.at[d], q_recv.at[d], plane(d)).wait_recv()
        own_rows(from_mate(d), 0)

    def attend(b, qb):
        def cols(kb, inside):
            tile(b, qb, kb, False)
            return inside

        lax.fori_loop(jnp.maximum(b * inner + qb - span, 0), inner, cols, 0)

    def middle(b):
        @pl.when(o >= b)
        def _():
            got_lift(b, False)

        @pl.when(has_above & (o >= b))
        def _():
            for copy in lift(b, False):
                copy.start()

    if outer > 1:
        got_down(1)
    if outer > 2:
        go_down(2)
    def whole_slot(b, carry):
        middle(b)
        return carry

    if back > 2:
        middle(1)
    elif back == 2:
        @pl.when(o >= 1)
        def _():
            got_lift(1, False)

        start_lift(1, True)
    elif back == 1:
        @pl.when(o >= 1)
        def _():
            got_lift(1, True)
    early = inner // 2 if back > 1 else 0

    def early_rows(qb, carry):
        attend(1, qb)
        return carry

    if early:
        @pl.when(o >= 1)
        def _():
            lax.fori_loop(inner - early, inner, early_rows, 0)

    if back > 2:
        lax.fori_loop(2, back - 1, whole_slot, 0)

        @pl.when(o >= back - 1)
        def _():
            got_lift(back - 1, False)

        start_lift(back - 1, True)
    if outer > 1:
        got_up(1)
    if outer > 2:
        go_up(2)

    def a_copy(qb, d):
        slot = a_all.at[qb, i]
        return remote(slot, slot, a_send.at[qb, d], a_recv.at[qb, d], plane(d))

    def send_rows(qb):
        for d in range(1, inner):
            a_copy(qb, d).start()

    def finish(qb):
        for r in range(group):
            cols = pl.ds(r * tok, tok)
            normal = acc[qb, :, cols] / row_total[qb, :, cols]
            a_all[qb, i, :, r * width : (r + 1) * width] = normal.T.astype(jnp.bfloat16)

    deepest = min(inner, span + inner - back * inner)

    def finish_rows(k, carry):
        qb = inner - 1 - k

        def slots(b, inside):
            attend(b, qb)
            return inside

        lax.fori_loop(jnp.where(k < early, 2, 1), jnp.minimum(o, back - 1) + 1, slots, 0)
        if back > 1:
            @pl.when((o >= back) & (qb == deepest - 1))
            def _():
                got_lift(back, True)

        if back >= 1:
            @pl.when((o >= back) & (qb < deepest))
            def _():
                attend(back, qb)

        finish(qb)
        send_rows(qb)
        return carry

    lax.fori_loop(0, inner, finish_rows, 0)

    def hop(t, carry):
        got_down(t - 1)
        go_down(t)
        got_up(t - 1)
        go_up(t)
        return carry

    if outer > 3:
        got_down(2)
        go_down(3)
        got_up(2)
        go_up(3)
        lax.fori_loop(4, outer, hop, 0)
    def multiply(qb, s):
        value = jnp.dot(a_all[qb, 0], w_all[s, 0:part_rows, :], preferred_element_type=jnp.float32)
        for j in range(1, inner):
            value += jnp.dot(
                a_all[qb, j], w_all[s, j * part_rows : (j + 1) * part_rows, :], preferred_element_type=jnp.float32
            )
        partial[s, qb] = value.astype(jnp.bfloat16)

    def p_copy(s):
        to = s // share
        d = (to + heads - head) % heads
        return remote(
            partial.at[s], peer.at[d, s % share], p_send.at[s], p_recv.at[d, s % share], {"head": to}
        )

    def give(s):
        @pl.when(s // share != head)
        def _():
            p_copy(s).start()

    def c_copy(sl, d):
        return remote(summed.at[sl, mate(d)], result.at[sl, i], c_send.at[sl, d], c_recv.at[sl, d], plane(d))

    def absorb(s):
        @pl.when(s // share == head)
        def _():
            sl = s % share
            for d in range(1, heads):
                slot = peer.at[d, sl]
                remote(slot, slot, p_send.at[s], p_recv.at[d, sl], {"head": (head + d) % heads}).wait_recv()

            def rows(j, carry):
                total = partial[s, j].astype(jnp.float32)
                for d in range(1, heads):
                    total = total + peer[d, sl, j].astype(jnp.float32)
                summed[sl, j] = total.astype(jnp.bfloat16)
                return carry

            lax.fori_loop(0, inner, rows, 0)
            for d in range(1, inner):
                c_copy(sl, d).start()
            result[sl, i] = summed[sl, i]

    def near(t, act):
        @pl.when(o - t >= 0)
        def _():
            act(jnp.maximum(o - t, 0))

        @pl.when((o + t < outer) & (t > 0))
        def _():
            act(jnp.minimum(o + t, outer - 1))

    near_count = max(outer - 1, 1)

    def got_rows(qb):
        for d in range(1, inner):
            slot = a_all.at[qb, from_mate(d)]
            remote(slot, slot, a_send.at[qb, d], a_recv.at[qb, d], plane(d)).wait_recv()

    def early_blocks(k, carry):
        qb = inner - 1 - k
        got_rows(qb)

        def shards(t, inside):
            near(t, lambda s: multiply(qb, s))
            return inside

        lax.fori_loop(0, near_count, shards, 0)
        return carry

    lax.fori_loop(0, inner - 1, early_blocks, 0)
    got_rows(0)

    def final_block(t, carry):
        def act(s):
            multiply(0, s)
            give(s)

        near(t, act)

        @pl.when(t >= 1)
        def _():
            near(t - 1, absorb)

        return carry

    lax.fori_loop(0, near_count, final_block, 0)
    near(near_count - 1, absorb)
    if outer > 1:
        if outer > 2:
            got_down(outer - 1)
            got_up(outer - 1)

        def far(s):
            def rows(qb, carry):
                multiply(qb, s)
                return carry

            lax.fori_loop(0, inner, rows, 0)
            give(s)

        near(outer - 1, far)
        near(outer - 1, absorb)
    for sl in range(share):
        for d in range(1, inner):
            slot = result.at[sl, from_mate(d)]
            remote(slot, slot, c_send.at[sl, d], c_recv.at[sl, d], plane(d)).wait_recv()
    wide = out_ref.shape[1] // (share * inner)
    for s in range(share):
        for j in range(inner):
            out_ref[:, (s * inner + j) * wide : (s * inner + j + 1) * wide] = result[s, j]

    for d in range(1, inner):
        for copy in kv_copies(d):
            copy.wait_send()
        q_copy(d).wait_send()
        for qb in range(inner):
            a_copy(qb, d).wait_send()
        for sl in range(share):
            c_copy(sl, d).wait_send()

    def given(s, carry):
        @pl.when(s // share != head)
        def _():
            p_copy(s).wait_send()

        return carry

    lax.fori_loop(0, outer, given, 0)

    def lift_done(b, only_last):
        @pl.when(has_above & (o >= b))
        def _():
            for copy in lift(b, only_last):
                copy.wait_send()

    if back > 1:
        def lift_sent(b, carry):
            lift_done(b, False)
            return carry

        lax.fori_loop(0, back - 1, lift_sent, 0)
    if back >= 1:
        lift_done(back - 1, True)

    def hop_sent(t, first):
        @pl.when(has_above & (o >= t - 1))
        def _():
            up_copy(t, first).wait_send()

        @pl.when(has_below & (o + t - 1 < outer))
        def _():
            down_copy(t, first).wait_send()

    def later_sent(t, carry):
        hop_sent(t, False)
        return carry

    if outer > 1:
        hop_sent(1, True)
        lax.fori_loop(2, outer, later_sent, 0)


def square_kernel(
    shape,
    q_in, k_in, v_in, w_ref, doc_ref, out_ref,
    lo_ref,
    q_ref, k_ref, v_ref,
    q_all, k_all, v_all, w_all, a_all, acc, row_max, row_total, partial, peer, summed, result,
    q_send, q_recv, k_send, k_recv, v_send, v_recv, kz_send, kz_recv, vz_send, vz_recv,
    up_send, up_recv, down_send, down_recv, a_send, a_recv, g_send, g_recv, p_send, p_recv, c_send, c_recv,
    hp_send, hp_recv, hc_send, hc_recv, local_sem,
):
    inner, outer, heads, group, back, span, last = shape
    tok, width = k_in.shape[0], k_in.shape[2]
    part_rows = group * width
    share = outer // heads
    seq, head = lax.axis_index("seq"), lax.axis_index("head")
    o, i = seq // inner, seq % inner
    ix, iy = i % 2, i // 2
    near_x, near_y = iy * 2 + 1 - ix, (1 - iy) * 2 + ix
    half = w_ref.shape[1] // 2

    def remote(src, dst, send, recv, device):
        return pltpu.make_async_remote_copy(
            src_ref=src, dst_ref=dst, send_sem=send, recv_sem=recv, device_id=device, device_id_type=MESH
        )

    def mate(d):
        return (i + d) % inner

    def plane(d):
        return {"seq": o * inner + mate(d)}

    above, below = {"seq": jnp.minimum(seq + inner, outer * inner - 1)}, {"seq": jnp.maximum(seq - inner, 0)}
    has_above, has_below = o + 1 < outer, o >= 1

    barrier = pltpu.get_barrier_semaphore()
    for d in range(1, inner):
        pl.semaphore_signal(barrier, inc=1, device_id=plane(d), device_id_type=MESH)
    for d in range(1, heads):
        pl.semaphore_signal(barrier, inc=1, device_id={"head": (head + d) % heads}, device_id_type=MESH)

    @pl.when(has_above)
    def _():
        pl.semaphore_signal(barrier, inc=1, device_id=above, device_id_type=MESH)

    @pl.when(has_below)
    def _():
        pl.semaphore_signal(barrier, inc=1, device_id=below, device_id_type=MESH)

    pl.semaphore_wait(
        barrier, inner - 1 + heads - 1 + has_above.astype(jnp.int32) + has_below.astype(jnp.int32)
    )

    def kv_copies(d):
        return (
            remote(k_ref.at[mate(d)], k_all.at[0, i], k_send.at[d], k_recv.at[d], plane(d)),
            remote(v_ref.at[mate(d)], v_all.at[0, i], v_send.at[d], v_recv.at[d], plane(d)),
        )

    def q_copy(d):
        return remote(q_ref.at[mate(d)], q_all.at[i], q_send.at[d], q_recv.at[d], plane(d))

    def slot_up(t, c):
        return w_all.at[jnp.maximum(o - t, 0), :, pl.ds(c * half, half)]

    def slot_down(t, c):
        return w_all.at[jnp.minimum(o + t, outer - 1), :, pl.ds(c * half, half)]

    def up_copy(t, c):
        src = w_ref.at[:, pl.ds(c * half, half)] if t == 1 else slot_up(t - 1, c)
        return remote(src, slot_up(t - 1, c), up_send.at[t, c], up_recv.at[t, c], above)

    def down_copy(t, c):
        src = w_ref.at[:, pl.ds(c * half, half)] if t == 1 else slot_down(t - 1, c)
        return remote(src, slot_down(t - 1, c), down_send.at[t, c], down_recv.at[t, c], below)

    def got_up(t, c):
        @pl.when(o >= t)
        def _():
            remote(slot_up(t, c), slot_up(t, c), up_send.at[t, c], up_recv.at[t, c], below).wait_recv()

    def got_down(t, c):
        @pl.when(o + t < outer)
        def _():
            remote(slot_down(t, c), slot_down(t, c), down_send.at[t, c], down_recv.at[t, c], above).wait_recv()

    def go_up(t, c):
        @pl.when(has_above & (o >= t - 1))
        def _():
            up_copy(t, c).start()

    def go_down(t, c):
        @pl.when(has_below & (o + t - 1 < outer))
        def _():
            down_copy(t, c).start()

    def pass_up(t, c):
        got_up(t, c)
        go_up(t + 1, c)

    def pass_down(t, c):
        got_down(t, c)
        go_down(t + 1, c)

    if outer > 1:
        go_up(1, 0)
        go_down(1, 0)
        go_down(1, 1)
    k_ref[...] = jnp.swapaxes(k_in[...], 0, 1)
    by_head = jnp.swapaxes(v_in[...], 0, 1)
    for j in range(inner):
        v_ref[j] = by_head[j].T
    by_head = jnp.swapaxes(q_in[...], 0, 1)
    for j in range(inner * group):
        q_ref[j // group, :, (j % group) * tok : (j % group + 1) * tok] = by_head[j].T
    for d in range(1, inner):
        for copy in kv_copies(d):
            copy.start()
    for d in range(1, inner):
        q_copy(d).start()

    locals_ = [
        pltpu.make_async_copy(q_ref.at[i], q_all.at[i], local_sem.at[0]),
        pltpu.make_async_copy(k_ref.at[i], k_all.at[0, i], local_sem.at[1]),
        pltpu.make_async_copy(v_ref.at[i], v_all.at[0, i], local_sem.at[2]),
        pltpu.make_async_copy(w_ref, w_all.at[o], local_sem.at[3]),
    ]
    for copy in locals_:
        copy.start()
    row_max[...] = jnp.full(row_max.shape, -1e30, jnp.float32)
    row_total[...] = jnp.zeros(row_total.shape, jnp.float32)
    acc[...] = jnp.zeros(acc.shape, jnp.float32)
    ends = [doc_ref[0]]
    for j in range(1, doc_ref.shape[0]):
        ends.append(ends[-1] + doc_ref[j])
    for qb in range(inner):
        row = (o * inner + qb) * tok + lax.broadcasted_iota(jnp.int32, (1, tok), 1)
        start = jnp.zeros((1, tok), jnp.int32)
        for end in ends:
            start = jnp.where(row >= end, end, start)
        lo_ref[qb] = start
    for copy in locals_:
        copy.wait()

    def from_mate(d):
        return (i + inner - d) % inner

    for d in range(1, inner):
        k_slot, v_slot = k_all.at[0, from_mate(d)], v_all.at[0, from_mate(d)]
        remote(k_slot, k_slot, k_send.at[d], k_recv.at[d], plane(d)).wait_recv()
        remote(v_slot, v_slot, v_send.at[d], v_recv.at[d], plane(d)).wait_recv()

    def slot_of(ref, b, only_last):
        return ref.at[b, pl.ds(inner - last, last)] if only_last else ref.at[b]

    def lift(b, only_last):
        return (
            remote(slot_of(k_all, b, only_last), slot_of(k_all, b + 1, only_last), kz_send.at[b], kz_recv.at[b + 1], above),
            remote(slot_of(v_all, b, only_last), slot_of(v_all, b + 1, only_last), vz_send.at[b], vz_recv.at[b + 1], above),
        )

    def start_lift(b, only_last):
        @pl.when(has_above & (o >= b))
        def _():
            for copy in lift(b, only_last):
                copy.start()

    def got_lift(b, only_last):
        k_slot, v_slot = slot_of(k_all, b, only_last), slot_of(v_all, b, only_last)
        remote(k_slot, k_slot, kz_send.at[b], kz_recv.at[b], below).wait_recv()
        remote(v_slot, v_slot, vz_send.at[b], vz_recv.at[b], below).wait_recv()

    if back >= 1:
        start_lift(0, back == 1)
    factor = math.log2(math.e) / math.sqrt(width)

    def tile(b, qb, kb, diagonal):
        key_pos = ((o - b) * inner + kb) * tok + lax.broadcasted_iota(jnp.int32, (tok, tok), 0)
        allowed = key_pos >= lo_ref[qb]
        if diagonal:
            allowed &= lax.broadcasted_iota(jnp.int32, (tok, tok), 0) <= lax.broadcasted_iota(
                jnp.int32, (tok, tok), 1
            )
        keys_here, values_here = k_all[b, kb], v_all[b, kb]
        raw = [
            jnp.dot(keys_here, q_all[qb, :, r * tok : (r + 1) * tok], preferred_element_type=jnp.float32)
            for r in range(group)
        ]
        for r in range(group):
            cols = pl.ds(r * tok, tok)
            scores = jnp.where(allowed, raw[r] * factor, -1e30)
            old_max = row_max[qb, :, cols]
            new_max = jnp.maximum(old_max, jnp.max(scores, axis=0, keepdims=True))
            weights = jnp.exp2(scores - new_max)
            rescale = jnp.exp2(old_max - new_max)
            row_max[qb, :, cols] = new_max
            row_total[qb, :, cols] = row_total[qb, :, cols] * rescale + jnp.sum(weights, axis=0, keepdims=True)
            acc[qb, :, cols] = acc[qb, :, cols] * rescale + jnp.dot(
                values_here, weights.astype(jnp.bfloat16), preferred_element_type=jnp.float32
            )

    def own_rows(qb, carry):
        tile(0, qb, qb, True)

        def own_keys(kb, inside):
            tile(0, qb, kb, False)
            return inside

        return lax.fori_loop(0, qb, own_keys, carry)

    own_rows(i, 0)

    @pl.when(o >= 1)
    def _():
        got_lift(1, False)

    start_lift(1, False)
    go_up(1, 1)
    for d in range(1, inner):
        q_slot = q_all.at[from_mate(d)]
        remote(q_slot, q_slot, q_send.at[d], q_recv.at[d], plane(d)).wait_recv()
        own_rows(from_mate(d), 0)
    for c in range(2):
        pass_down(1, c)
    pass_up(1, 0)

    def attend(b, qb):
        def cols(kb, inside):
            tile(b, qb, kb, False)
            return inside

        lax.fori_loop(jnp.maximum(b * inner + qb - span, 0), inner, cols, 0)

    def early_rows(k, carry):
        attend(1, inner - 1 - k)
        return carry

    @pl.when(o >= 1)
    def _():
        lax.fori_loop(0, inner, early_rows, 0)

    @pl.when(o >= 2)
    def _():
        got_lift(2, False)

    start_lift(2, True)
    pass_up(1, 1)

    def a_copy(qb, k):
        slot = a_all.at[qb, i]
        to = {"seq": o * inner + (near_x if k == 0 else near_y)}
        return remote(slot, slot, a_send.at[qb, k], a_recv.at[qb, k], to)

    def send_rows(qb):
        for k in range(2):
            a_copy(qb, k).start()

    def got_near(qb, k):
        slot = a_all.at[qb, near_x if k == 0 else near_y]
        remote(slot, slot, a_send.at[qb, k], a_recv.at[qb, k], plane(1)).wait_recv()

    def relay(qb, k):
        slot = a_all.at[qb, near_x if k == 0 else near_y, pl.ds(k * (tok // 2), tok // 2)]
        to = {"seq": o * inner + (near_y if k == 0 else near_x)}
        return remote(slot, slot, g_send.at[qb, k], g_recv.at[qb, k], to)

    def got_rows(qb):
        for k in range(2):
            slot = a_all.at[qb, inner - 1 - i, pl.ds(k * (tok // 2), tok // 2)]
            remote(slot, slot, g_send.at[qb, k], g_recv.at[qb, k], plane(1)).wait_recv()

    def finish(qb):
        for r in range(group):
            cols = pl.ds(r * tok, tok)
            normal = acc[qb, :, cols] / row_total[qb, :, cols]
            a_all[qb, i, :, r * width : (r + 1) * width] = normal.T.astype(jnp.bfloat16)

    deepest = min(inner, span + inner - back * inner)

    def finish_rows(k, carry):
        qb = inner - 1 - k

        def slots(b, inside):
            attend(b, qb)
            return inside

        lax.fori_loop(2, jnp.minimum(o, back - 1) + 1, slots, 0)
        if back > 1:
            @pl.when((o >= back) & (qb == deepest - 1))
            def _():
                got_lift(back, True)

        if back >= 1:
            @pl.when((o >= back) & (qb < deepest))
            def _():
                attend(back, qb)

        finish(qb)
        send_rows(qb)
        return carry

    lax.fori_loop(0, inner, finish_rows, 0)

    def pass_rows(qb):
        for k in range(2):
            got_near(qb, k)
            relay(qb, k).start()

    pass_rows(inner - 1)
    for c in range(2):
        pass_down(2, c)
    pass_up(2, 0)
    for qb in range(inner - 2, -1, -1):
        pass_rows(qb)
    pass_up(2, 1)

    def multiply(qb, s, cols=slice(None)):
        value = jnp.dot(a_all[qb, 0], w_all[s, 0:part_rows, cols], preferred_element_type=jnp.float32)
        for j in range(1, inner):
            value += jnp.dot(
                a_all[qb, j], w_all[s, j * part_rows : (j + 1) * part_rows, cols], preferred_element_type=jnp.float32
            )
        partial[s, qb, :, cols] = value.astype(jnp.bfloat16)

    def columns(c):
        return pl.ds(0, 2 * half) if c is None else pl.ds(c * half, half)

    def p_copy(s, c=None):
        to = s // share
        d = (to + heads - head) % heads
        sl = s % share
        src, dst = partial.at[s, :, :, columns(c)], peer.at[d, sl, :, :, columns(c)]
        if c is None:
            return remote(src, dst, p_send.at[s], p_recv.at[d, sl], {"head": to})
        return remote(src, dst, hp_send.at[c], hp_recv.at[c], {"head": to})

    def give(s, c=None):
        @pl.when(s // share != head)
        def _():
            p_copy(s, c).start()

    def c_copy(sl, d, c=None):
        src, dst = summed.at[sl, mate(d), :, columns(c)], result.at[sl, i, :, columns(c)]
        if c is None:
            return remote(src, dst, c_send.at[sl, d], c_recv.at[sl, d], plane(d))
        return remote(src, dst, hc_send.at[c, d], hc_recv.at[c, d], plane(d))

    def absorb(s, c=None):
        @pl.when(s // share == head)
        def _():
            sl = s % share
            cols = columns(c)
            for d in range(1, heads):
                slot = peer.at[d, sl, :, :, cols]
                if c is None:
                    arrived = p_recv.at[d, sl]
                else:
                    arrived = hp_recv.at[c]
                remote(slot, slot, p_send.at[s], arrived, {"head": (head + d) % heads}).wait_recv()

            def rows(j, carry):
                total = partial[s, j, :, cols].astype(jnp.float32)
                for d in range(1, heads):
                    total = total + peer[d, sl, j, :, cols].astype(jnp.float32)
                summed[sl, j, :, cols] = total.astype(jnp.bfloat16)
                return carry

            lax.fori_loop(0, inner, rows, 0)
            for d in range(1, inner):
                c_copy(sl, d, c).start()
            result[sl, i, :, cols] = summed[sl, i, :, cols]

    def near(t, act):
        @pl.when(o - t >= 0)
        def _():
            act(jnp.maximum(o - t, 0))

        @pl.when((o + t < outer) & (t > 0))
        def _():
            act(jnp.minimum(o + t, outer - 1))

    near_count = max(outer - 1, 1)

    def early_blocks(k, carry):
        qb = inner - 1 - k
        got_rows(qb)

        def shards(t, inside):
            near(t, lambda s: multiply(qb, s))
            return inside

        lax.fori_loop(0, near_count, shards, 0)
        return carry

    lax.fori_loop(0, inner - 1, early_blocks, 0)
    got_rows(0)

    def final_block(t, carry):
        def act(s):
            multiply(0, s)
            give(s)

        near(t, act)

        @pl.when(t >= 1)
        def _():
            near(t - 1, absorb)

        return carry

    lax.fori_loop(0, near_count, final_block, 0)
    near(near_count - 1, absorb)
    for c in range(2):
        got_down(outer - 1, c)
        got_up(outer - 1, c)

        def far(s):
            def rows(qb, carry):
                multiply(qb, s, pl.ds(c * half, half))
                return carry

            lax.fori_loop(0, inner, rows, 0)
            give(s, c)

        near(outer - 1, far)
        near(outer - 1, lambda s: absorb(s, c))

    def is_far(s):
        return (s - o == outer - 1) | (o - s == outer - 1)

    for sl in range(share):
        for d in range(1, inner):
            @pl.when(is_far(head * share + sl))
            def _():
                for c in range(2):
                    slot = result.at[sl, from_mate(d), :, columns(c)]
                    remote(slot, slot, hc_send.at[c, d], hc_recv.at[c, d], plane(d)).wait_recv()

            @pl.when(jnp.logical_not(is_far(head * share + sl)))
            def _():
                slot = result.at[sl, from_mate(d)]
                remote(slot, slot, c_send.at[sl, d], c_recv.at[sl, d], plane(d)).wait_recv()

    wide = out_ref.shape[1] // (share * inner)
    for s in range(share):
        for j in range(inner):
            out_ref[:, (s * inner + j) * wide : (s * inner + j + 1) * wide] = result[s, j]

    for d in range(1, inner):
        for copy in kv_copies(d):
            copy.wait_send()
        q_copy(d).wait_send()
        for sl in range(share):
            @pl.when(is_far(head * share + sl))
            def _():
                for c in range(2):
                    c_copy(sl, d, c).wait_send()

            @pl.when(jnp.logical_not(is_far(head * share + sl)))
            def _():
                c_copy(sl, d).wait_send()

    for qb in range(inner):
        for k in range(2):
            a_copy(qb, k).wait_send()
            relay(qb, k).wait_send()

    def given(s, carry):
        @pl.when((s // share != head) & is_far(s))
        def _():
            for c in range(2):
                p_copy(s, c).wait_send()

        @pl.when((s // share != head) & jnp.logical_not(is_far(s)))
        def _():
            p_copy(s).wait_send()

        return carry

    lax.fori_loop(0, outer, given, 0)

    for b in range(back):
        @pl.when(has_above & (o >= b))
        def _():
            for copy in lift(b, b == back - 1):
                copy.wait_send()

    for t in range(1, outer):
        for c in range(2):
            @pl.when(has_above & (o >= t - 1))
            def _():
                up_copy(t, c).wait_send()

            @pl.when(has_below & (o + t - 1 < outer))
            def _():
                down_copy(t, c).wait_send()


def body(queries, keys, values, out_weight, doc_lengths):
    tok, heads_here, width = queries.shape
    inner = keys.shape[1]
    group = heads_here // inner
    count = lax.axis_size("seq")
    heads = lax.axis_size("head")
    outer = count // inner
    span = count // 2 + 1
    plane_rows = inner * tok
    reach = span * tok - 1
    back = min(outer - 1, -(-reach // plane_rows))
    last = min(inner, -(-(reach - (back - 1) * plane_rows) // tok))
    share = outer // heads
    depth, wide = out_weight.shape

    positions = (lax.axis_index("seq") // inner) * plane_rows + jnp.arange(plane_rows, dtype=jnp.int32)
    ends = jnp.cumsum(doc_lengths)
    starts = jnp.max(jnp.where(ends[None, :] <= positions[:, None], ends[None, :], 0), axis=1)
    starts = starts.reshape(inner, 1, tok)

    bf16, f32 = jnp.bfloat16, jnp.float32
    dma = pltpu.SemaphoreType.DMA
    scratch = [
        pltpu.VMEM((inner, width, group * tok), bf16),
        pltpu.VMEM((inner, tok, width), bf16),
        pltpu.VMEM((inner, width, tok), bf16),
        pltpu.VMEM((inner, width, group * tok), bf16),
        pltpu.VMEM((back + 1, inner, tok, width), bf16),
        pltpu.VMEM((back + 1, inner, width, tok), bf16),
        pltpu.VMEM((outer, depth, wide), bf16),
        pltpu.VMEM((inner, inner, tok, group * width), bf16),
        pltpu.VMEM((inner, width, group * tok), f32),
        pltpu.VMEM((inner, 1, group * tok), f32),
        pltpu.VMEM((inner, 1, group * tok), f32),
        pltpu.VMEM((outer, inner, tok, wide), bf16),
        pltpu.VMEM((heads, share, inner, tok, wide), bf16),
        pltpu.VMEM((share, inner, tok, wide), bf16),
        pltpu.VMEM((share, inner, tok, wide), bf16),
    ]
    scratch += [dma((inner,))] * 6 + [dma((back + 1,))] * 4 + [dma((outer,))] * 4
    scratch += [dma((inner, inner))] * 2 + [dma((outer,)), dma((heads, share))] + [dma((share, inner))] * 2 + [dma((4,))]
    shape = (inner, outer, heads, group, back, span, last)
    vmem = pl.BlockSpec(memory_space=pltpu.VMEM)
    run, last_in, last_spec = kernel, starts, vmem
    if inner == 4 and outer == 4 and back == 3:
        run, last_in, last_spec = square_kernel, doc_lengths, pl.BlockSpec(memory_space=pltpu.SMEM)
        scratch = [pltpu.VMEM((inner, 1, tok), jnp.int32)] + scratch[:15]
        scratch += [dma((inner,))] * 6 + [dma((back + 1,))] * 4 + [dma((outer, 2))] * 4
        scratch += [dma((inner, 2))] * 4 + [dma((outer,)), dma((heads, share))] + [dma((share, inner))] * 2
        scratch += [dma((2,))] * 2 + [dma((2, inner))] * 2 + [dma((4,))]
    return pl.pallas_call(
        functools.partial(run, shape),
        out_shape=jax.ShapeDtypeStruct((tok, share * inner * wide), bf16),
        in_specs=[vmem] * 4 + [last_spec],
        out_specs=vmem,
        scratch_shapes=scratch,
        compiler_params=pltpu.CompilerParams(
            collective_id=0, has_side_effects=True, vmem_limit_bytes=60 * 1024 * 1024
        ),
    )(queries, keys, values, out_weight, last_in)


def solution(mesh):
    placed = (
        P("seq", "head", None),
        P("seq", "head", None),
        P("seq", "head", None),
        P("head", "seq"),
        P(),
    )
    return jax.shard_map(
        body, mesh=mesh, in_specs=placed, out_specs=P("seq", "head"), check_vma=False
    )
```

```python
import functools
import math

import jax
import jax.numpy as jnp
from jax import lax
from jax.experimental import pallas as pl
from jax.experimental.pallas import tpu as pltpu
from jax.sharding import PartitionSpec as P

MESH = pl.DeviceIdType.MESH


def kernel(
    shape,
    q_in, k_in, v_in, w_ref, lo_ref, out_ref,
    q_ref, k_ref, v_ref,
    q_all, k_all, v_all, w_all, a_all, acc, row_max, row_total, partial, peer, summed, result,
    q_send, q_recv, k_send, k_recv, v_send, v_recv, kz_send, kz_recv, vz_send, vz_recv,
    up_send, up_recv, down_send, down_recv, a_send, a_recv, p_send, p_recv, c_send, c_recv, local_sem,
):
    inner, outer, heads, group, back, span, last = shape
    tok, width = k_in.shape[0], k_in.shape[2]
    part_rows = group * width
    share = outer // heads
    seq, head = lax.axis_index("seq"), lax.axis_index("head")
    o, i = seq // inner, seq % inner

    def remote(src, dst, send, recv, device):
        return pltpu.make_async_remote_copy(
            src_ref=src, dst_ref=dst, send_sem=send, recv_sem=recv, device_id=device, device_id_type=MESH
        )

    def mate(d):
        return (i + d) % inner

    def plane(d):
        return {"seq": o * inner + mate(d)}

    above, below = {"seq": jnp.minimum(seq + inner, outer * inner - 1)}, {"seq": jnp.maximum(seq - inner, 0)}
    has_above, has_below = o + 1 < outer, o >= 1

    barrier = pltpu.get_barrier_semaphore()
    for d in range(1, inner):
        pl.semaphore_signal(barrier, inc=1, device_id=plane(d), device_id_type=MESH)
    for d in range(1, heads):
        pl.semaphore_signal(barrier, inc=1, device_id={"head": (head + d) % heads}, device_id_type=MESH)

    @pl.when(has_above)
    def _():
        pl.semaphore_signal(barrier, inc=1, device_id=above, device_id_type=MESH)

    @pl.when(has_below)
    def _():
        pl.semaphore_signal(barrier, inc=1, device_id=below, device_id_type=MESH)

    pl.semaphore_wait(
        barrier, inner - 1 + heads - 1 + has_above.astype(jnp.int32) + has_below.astype(jnp.int32)
    )

    def kv_copies(d):
        return (
            remote(k_ref.at[mate(d)], k_all.at[0, i], k_send.at[d], k_recv.at[d], plane(d)),
            remote(v_ref.at[mate(d)], v_all.at[0, i], v_send.at[d], v_recv.at[d], plane(d)),
        )

    def q_copy(d):
        return remote(q_ref.at[mate(d)], q_all.at[i], q_send.at[d], q_recv.at[d], plane(d))

    def up_copy(t, first):
        return remote(
            w_ref if first else w_all.at[jnp.maximum(o - t + 1, 0)],
            w_all.at[jnp.maximum(o - t + 1, 0)], up_send.at[t], up_recv.at[t], above,
        )

    def down_copy(t, first):
        return remote(
            w_ref if first else w_all.at[jnp.minimum(o + t - 1, outer - 1)],
            w_all.at[jnp.minimum(o + t - 1, outer - 1)], down_send.at[t], down_recv.at[t], below,
        )

    def got_up(t):
        @pl.when(o >= t)
        def _():
            slot = w_all.at[jnp.maximum(o - t, 0)]
            remote(slot, slot, up_send.at[t], up_recv.at[t], below).wait_recv()

    def got_down(t):
        @pl.when(o + t < outer)
        def _():
            slot = w_all.at[jnp.minimum(o + t, outer - 1)]
            remote(slot, slot, down_send.at[t], down_recv.at[t], above).wait_recv()

    def go_up(t, first=False):
        @pl.when(has_above & (o >= t - 1))
        def _():
            up_copy(t, first).start()

    def go_down(t, first=False):
        @pl.when(has_below & (o + t - 1 < outer))
        def _():
            down_copy(t, first).start()

    if outer > 1:
        go_up(1, True)
        go_down(1, True)
    k_ref[...] = jnp.swapaxes(k_in[...], 0, 1)
    by_head = jnp.swapaxes(v_in[...], 0, 1)
    for j in range(inner):
        v_ref[j] = by_head[j].T
    by_head = jnp.swapaxes(q_in[...], 0, 1)
    for j in range(inner * group):
        q_ref[j // group, :, (j % group) * tok : (j % group + 1) * tok] = by_head[j].T
    for d in range(1, inner):
        for copy in kv_copies(d):
            copy.start()
    for d in range(1, inner):
        q_copy(d).start()

    locals_ = [
        pltpu.make_async_copy(q_ref.at[i], q_all.at[i], local_sem.at[0]),
        pltpu.make_async_copy(k_ref.at[i], k_all.at[0, i], local_sem.at[1]),
        pltpu.make_async_copy(v_ref.at[i], v_all.at[0, i], local_sem.at[2]),
        pltpu.make_async_copy(w_ref, w_all.at[o], local_sem.at[3]),
    ]
    for copy in locals_:
        copy.start()
    for copy in locals_:
        copy.wait()

    def from_mate(d):
        return (i + inner - d) % inner

    for d in range(1, inner):
        k_slot, v_slot = k_all.at[0, from_mate(d)], v_all.at[0, from_mate(d)]
        remote(k_slot, k_slot, k_send.at[d], k_recv.at[d], plane(d)).wait_recv()
        remote(v_slot, v_slot, v_send.at[d], v_recv.at[d], plane(d)).wait_recv()

    def slot_of(ref, b, only_last):
        return ref.at[b, pl.ds(inner - last, last)] if only_last else ref.at[b]

    def lift(b, only_last):
        return (
            remote(slot_of(k_all, b, only_last), slot_of(k_all, b + 1, only_last), kz_send.at[b], kz_recv.at[b + 1], above),
            remote(slot_of(v_all, b, only_last), slot_of(v_all, b + 1, only_last), vz_send.at[b], vz_recv.at[b + 1], above),
        )

    def start_lift(b, only_last):
        @pl.when(has_above & (o >= b))
        def _():
            for copy in lift(b, only_last):
                copy.start()

    def got_lift(b, only_last):
        k_slot, v_slot = slot_of(k_all, b, only_last), slot_of(v_all, b, only_last)
        remote(k_slot, k_slot, kz_send.at[b], kz_recv.at[b], below).wait_recv()
        remote(v_slot, v_slot, vz_send.at[b], vz_recv.at[b], below).wait_recv()

    if back >= 1:
        start_lift(0, back == 1)
    row_max[...] = jnp.full(row_max.shape, -1e30, jnp.float32)
    row_total[...] = jnp.zeros(row_total.shape, jnp.float32)
    acc[...] = jnp.zeros(acc.shape, jnp.float32)
    factor = math.log2(math.e) / math.sqrt(width)

    def tile(b, qb, kb, diagonal):
        key_pos = ((o - b) * inner + kb) * tok + lax.broadcasted_iota(jnp.int32, (tok, tok), 0)
        allowed = key_pos >= lo_ref[qb]
        if diagonal:
            allowed &= lax.broadcasted_iota(jnp.int32, (tok, tok), 0) <= lax.broadcasted_iota(
                jnp.int32, (tok, tok), 1
            )
        keys_here, values_here = k_all[b, kb], v_all[b, kb]
        raw = [
            jnp.dot(keys_here, q_all[qb, :, r * tok : (r + 1) * tok], preferred_element_type=jnp.float32)
            for r in range(group)
        ]
        for r in range(group):
            cols = pl.ds(r * tok, tok)
            scores = jnp.where(allowed, raw[r] * factor, -1e30)
            old_max = row_max[qb, :, cols]
            new_max = jnp.maximum(old_max, jnp.max(scores, axis=0, keepdims=True))
            weights = jnp.exp2(scores - new_max)
            rescale = jnp.exp2(old_max - new_max)
            row_max[qb, :, cols] = new_max
            row_total[qb, :, cols] = row_total[qb, :, cols] * rescale + jnp.sum(weights, axis=0, keepdims=True)
            acc[qb, :, cols] = acc[qb, :, cols] * rescale + jnp.dot(
                values_here, weights.astype(jnp.bfloat16), preferred_element_type=jnp.float32
            )

    def own_rows(qb, carry):
        tile(0, qb, qb, True)

        def own_keys(kb, inside):
            tile(0, qb, kb, False)
            return inside

        return lax.fori_loop(0, qb, own_keys, carry)

    own_rows(i, 0)
    for d in range(1, inner):
        q_slot = q_all.at[from_mate(d)]
        remote(q_slot, q_slot, q_send.at[d], q_recv.at[d], plane(d)).wait_recv()
        own_rows(from_mate(d), 0)

    def attend(b, qb):
        def cols(kb, inside):
            tile(b, qb, kb, False)
            return inside

        lax.fori_loop(jnp.maximum(b * inner + qb - span, 0), inner, cols, 0)

    def middle(b):
        @pl.when(o >= b)
        def _():
            got_lift(b, False)

        @pl.when(has_above & (o >= b))
        def _():
            for copy in lift(b, False):
                copy.start()

    if outer > 1:
        got_down(1)
    if outer > 2:
        go_down(2)
    def whole_slot(b, carry):
        middle(b)
        return carry

    if back > 2:
        middle(1)
    elif back == 2:
        @pl.when(o >= 1)
        def _():
            got_lift(1, False)

        start_lift(1, True)
    elif back == 1:
        @pl.when(o >= 1)
        def _():
            got_lift(1, True)
    early = inner // 2 if back > 1 else 0

    def early_rows(qb, carry):
        attend(1, qb)
        return carry

    if early:
        @pl.when(o >= 1)
        def _():
            lax.fori_loop(inner - early, inner, early_rows, 0)

    if back > 2:
        lax.fori_loop(2, back - 1, whole_slot, 0)

        @pl.when(o >= back - 1)
        def _():
            got_lift(back - 1, False)

        start_lift(back - 1, True)
    if outer > 1:
        got_up(1)
    if outer > 2:
        go_up(2)

    def a_copy(qb, d):
        slot = a_all.at[qb, i]
        return remote(slot, slot, a_send.at[qb, d], a_recv.at[qb, d], plane(d))

    def send_rows(qb):
        for d in range(1, inner):
            a_copy(qb, d).start()

    def finish(qb):
        for r in range(group):
            cols = pl.ds(r * tok, tok)
            normal = acc[qb, :, cols] / row_total[qb, :, cols]
            a_all[qb, i, :, r * width : (r + 1) * width] = normal.T.astype(jnp.bfloat16)

    deepest = min(inner, span + inner - back * inner)

    def finish_rows(k, carry):
        qb = inner - 1 - k

        def slots(b, inside):
            attend(b, qb)
            return inside

        lax.fori_loop(jnp.where(k < early, 2, 1), jnp.minimum(o, back - 1) + 1, slots, 0)
        if back > 1:
            @pl.when((o >= back) & (qb == deepest - 1))
            def _():
                got_lift(back, True)

        if back >= 1:
            @pl.when((o >= back) & (qb < deepest))
            def _():
                attend(back, qb)

        finish(qb)
        send_rows(qb)
        return carry

    lax.fori_loop(0, inner, finish_rows, 0)

    def hop(t, carry):
        got_down(t - 1)
        go_down(t)
        got_up(t - 1)
        go_up(t)
        return carry

    if outer > 3:
        got_down(2)
        go_down(3)
        got_up(2)
        go_up(3)
        lax.fori_loop(4, outer, hop, 0)
    def multiply(qb, s):
        value = jnp.dot(a_all[qb, 0], w_all[s, 0:part_rows, :], preferred_element_type=jnp.float32)
        for j in range(1, inner):
            value += jnp.dot(
                a_all[qb, j], w_all[s, j * part_rows : (j + 1) * part_rows, :], preferred_element_type=jnp.float32
            )
        partial[s, qb] = value.astype(jnp.bfloat16)

    def p_copy(s):
        to = s // share
        d = (to + heads - head) % heads
        return remote(
            partial.at[s], peer.at[d, s % share], p_send.at[s], p_recv.at[d, s % share], {"head": to}
        )

    def give(s):
        @pl.when(s // share != head)
        def _():
            p_copy(s).start()

    def c_copy(sl, d):
        return remote(summed.at[sl, mate(d)], result.at[sl, i], c_send.at[sl, d], c_recv.at[sl, d], plane(d))

    def absorb(s):
        @pl.when(s // share == head)
        def _():
            sl = s % share
            for d in range(1, heads):
                slot = peer.at[d, sl]
                remote(slot, slot, p_send.at[s], p_recv.at[d, sl], {"head": (head + d) % heads}).wait_recv()

            def rows(j, carry):
                total = partial[s, j].astype(jnp.float32)
                for d in range(1, heads):
                    total = total + peer[d, sl, j].astype(jnp.float32)
                summed[sl, j] = total.astype(jnp.bfloat16)
                return carry

            lax.fori_loop(0, inner, rows, 0)
            for d in range(1, inner):
                c_copy(sl, d).start()
            result[sl, i] = summed[sl, i]

    def near(t, act):
        @pl.when(o - t >= 0)
        def _():
            act(jnp.maximum(o - t, 0))

        @pl.when((o + t < outer) & (t > 0))
        def _():
            act(jnp.minimum(o + t, outer - 1))

    near_count = max(outer - 1, 1)

    def got_rows(qb):
        for d in range(1, inner):
            slot = a_all.at[qb, from_mate(d)]
            remote(slot, slot, a_send.at[qb, d], a_recv.at[qb, d], plane(d)).wait_recv()

    def early_blocks(k, carry):
        qb = inner - 1 - k
        got_rows(qb)

        def shards(t, inside):
            near(t, lambda s: multiply(qb, s))
            return inside

        lax.fori_loop(0, near_count, shards, 0)
        return carry

    lax.fori_loop(0, inner - 1, early_blocks, 0)
    got_rows(0)

    def final_block(t, carry):
        def act(s):
            multiply(0, s)
            give(s)

        near(t, act)

        @pl.when(t >= 1)
        def _():
            near(t - 1, absorb)

        return carry

    lax.fori_loop(0, near_count, final_block, 0)
    near(near_count - 1, absorb)
    if outer > 1:
        if outer > 2:
            got_down(outer - 1)
            got_up(outer - 1)

        def far(s):
            def rows(qb, carry):
                multiply(qb, s)
                return carry

            lax.fori_loop(0, inner, rows, 0)
            give(s)

        near(outer - 1, far)
        near(outer - 1, absorb)
    for sl in range(share):
        for d in range(1, inner):
            slot = result.at[sl, from_mate(d)]
            remote(slot, slot, c_send.at[sl, d], c_recv.at[sl, d], plane(d)).wait_recv()
    wide = out_ref.shape[1] // (share * inner)
    for s in range(share):
        for j in range(inner):
            out_ref[:, (s * inner + j) * wide : (s * inner + j + 1) * wide] = result[s, j]

    for d in range(1, inner):
        for copy in kv_copies(d):
            copy.wait_send()
        q_copy(d).wait_send()
        for qb in range(inner):
            a_copy(qb, d).wait_send()
        for sl in range(share):
            c_copy(sl, d).wait_send()

    def given(s, carry):
        @pl.when(s // share != head)
        def _():
            p_copy(s).wait_send()

        return carry

    lax.fori_loop(0, outer, given, 0)

    def lift_done(b, only_last):
        @pl.when(has_above & (o >= b))
        def _():
            for copy in lift(b, only_last):
                copy.wait_send()

    if back > 1:
        def lift_sent(b, carry):
            lift_done(b, False)
            return carry

        lax.fori_loop(0, back - 1, lift_sent, 0)
    if back >= 1:
        lift_done(back - 1, True)

    def hop_sent(t, first):
        @pl.when(has_above & (o >= t - 1))
        def _():
            up_copy(t, first).wait_send()

        @pl.when(has_below & (o + t - 1 < outer))
        def _():
            down_copy(t, first).wait_send()

    def later_sent(t, carry):
        hop_sent(t, False)
        return carry

    if outer > 1:
        hop_sent(1, True)
        lax.fori_loop(2, outer, later_sent, 0)


def square_kernel(
    shape,
    q_hbm, k_hbm, v_hbm, w_hbm, doc_ref, out_ref,
    q_in, k_in, v_in, w_ref, lo_ref,
    q_ref, k_ref, v_ref,
    q_all, k_all, v_all, w_all, a_all, acc, row_max, row_total, partial, peer, summed, result,
    q_send, q_recv, k_send, k_recv, v_send, v_recv, kz_send, kz_recv, vz_send, vz_recv,
    up_send, up_recv, down_send, down_recv, a_send, a_recv, g_send, g_recv, p_send, p_recv, c_send, c_recv,
    hp_send, hp_recv, hc_send, hc_recv, in_sem, local_sem,
):
    inner, outer, heads, group, back, span, last = shape
    tok, width = k_in.shape[0], k_in.shape[2]
    part_rows = group * width
    share = outer // heads
    seq, head = lax.axis_index("seq"), lax.axis_index("head")
    o, i = seq // inner, seq % inner
    ix, iy = i % 2, i // 2
    near_x, near_y = iy * 2 + 1 - ix, (1 - iy) * 2 + ix
    half = w_ref.shape[1] // 2

    def remote(src, dst, send, recv, device):
        return pltpu.make_async_remote_copy(
            src_ref=src, dst_ref=dst, send_sem=send, recv_sem=recv, device_id=device, device_id_type=MESH
        )

    def mate(d):
        return (i + d) % inner

    def plane(d):
        return {"seq": o * inner + mate(d)}

    above, below = {"seq": jnp.minimum(seq + inner, outer * inner - 1)}, {"seq": jnp.maximum(seq - inner, 0)}
    has_above, has_below = o + 1 < outer, o >= 1

    fetch_w, fetch_k, fetch_v, fetch_q = (
        pltpu.make_async_copy(src, dst, in_sem.at[j])
        for j, (src, dst) in enumerate(((w_hbm, w_ref), (k_hbm, k_in), (v_hbm, v_in), (q_hbm, q_in)))
    )
    for fetch in (fetch_w, fetch_k, fetch_v, fetch_q):
        fetch.start()

    barrier = pltpu.get_barrier_semaphore()
    for d in range(1, inner):
        pl.semaphore_signal(barrier, inc=1, device_id=plane(d), device_id_type=MESH)
    for d in range(1, heads):
        pl.semaphore_signal(barrier, inc=1, device_id={"head": (head + d) % heads}, device_id_type=MESH)

    @pl.when(has_above)
    def _():
        pl.semaphore_signal(barrier, inc=1, device_id=above, device_id_type=MESH)

    @pl.when(has_below)
    def _():
        pl.semaphore_signal(barrier, inc=1, device_id=below, device_id_type=MESH)

    pl.semaphore_wait(
        barrier, inner - 1 + heads - 1 + has_above.astype(jnp.int32) + has_below.astype(jnp.int32)
    )

    def kv_copies(d):
        return (
            remote(k_ref.at[mate(d)], k_all.at[0, i], k_send.at[d], k_recv.at[d], plane(d)),
            remote(v_ref.at[mate(d)], v_all.at[0, i], v_send.at[d], v_recv.at[d], plane(d)),
        )

    def q_copy(d):
        return remote(q_ref.at[mate(d)], q_all.at[i], q_send.at[d], q_recv.at[d], plane(d))

    def slot_up(t, c):
        return w_all.at[jnp.maximum(o - t, 0), :, pl.ds(c * half, half)]

    def slot_down(t, c):
        return w_all.at[jnp.minimum(o + t, outer - 1), :, pl.ds(c * half, half)]

    def up_copy(t, c):
        src = w_ref.at[:, pl.ds(c * half, half)] if t == 1 else slot_up(t - 1, c)
        return remote(src, slot_up(t - 1, c), up_send.at[t, c], up_recv.at[t, c], above)

    def down_copy(t, c):
        src = w_ref.at[:, pl.ds(c * half, half)] if t == 1 else slot_down(t - 1, c)
        return remote(src, slot_down(t - 1, c), down_send.at[t, c], down_recv.at[t, c], below)

    def got_up(t, c):
        @pl.when(o >= t)
        def _():
            remote(slot_up(t, c), slot_up(t, c), up_send.at[t, c], up_recv.at[t, c], below).wait_recv()

    def got_down(t, c):
        @pl.when(o + t < outer)
        def _():
            remote(slot_down(t, c), slot_down(t, c), down_send.at[t, c], down_recv.at[t, c], above).wait_recv()

    def go_up(t, c):
        @pl.when(has_above & (o >= t - 1))
        def _():
            up_copy(t, c).start()

    def go_down(t, c):
        @pl.when(has_below & (o + t - 1 < outer))
        def _():
            down_copy(t, c).start()

    def pass_up(t, c):
        got_up(t, c)
        go_up(t + 1, c)

    def pass_down(t, c):
        got_down(t, c)
        go_down(t + 1, c)

    if outer > 1:
        fetch_w.wait()
        go_up(1, 0)
        go_down(1, 0)
        go_down(1, 1)
    fetch_k.wait()
    k_ref[...] = jnp.swapaxes(k_in[...], 0, 1)
    fetch_v.wait()
    by_head = jnp.swapaxes(v_in[...], 0, 1)
    for j in range(inner):
        v_ref[j] = by_head[j].T
    for d in range(1, inner):
        for copy in kv_copies(d):
            copy.start()
    fetch_q.wait()
    by_head = jnp.swapaxes(q_in[...], 0, 1)
    for j in range(inner * group):
        q_ref[j // group, :, (j % group) * tok : (j % group + 1) * tok] = by_head[j].T
    for d in range(1, inner):
        q_copy(d).start()

    locals_ = [
        pltpu.make_async_copy(q_ref.at[i], q_all.at[i], local_sem.at[0]),
        pltpu.make_async_copy(k_ref.at[i], k_all.at[0, i], local_sem.at[1]),
        pltpu.make_async_copy(v_ref.at[i], v_all.at[0, i], local_sem.at[2]),
        pltpu.make_async_copy(w_ref, w_all.at[o], local_sem.at[3]),
    ]
    for copy in locals_:
        copy.start()
    row_max[...] = jnp.full(row_max.shape, -1e30, jnp.float32)
    row_total[...] = jnp.zeros(row_total.shape, jnp.float32)
    acc[...] = jnp.zeros(acc.shape, jnp.float32)
    ends = [doc_ref[0]]
    for j in range(1, doc_ref.shape[0]):
        ends.append(ends[-1] + doc_ref[j])
    for qb in range(inner):
        row = (o * inner + qb) * tok + lax.broadcasted_iota(jnp.int32, (1, tok), 1)
        start = jnp.zeros((1, tok), jnp.int32)
        for end in ends:
            start = jnp.where(row >= end, end, start)
        lo_ref[qb] = start
    for copy in locals_:
        copy.wait()

    def from_mate(d):
        return (i + inner - d) % inner

    for d in range(1, inner):
        k_slot, v_slot = k_all.at[0, from_mate(d)], v_all.at[0, from_mate(d)]
        remote(k_slot, k_slot, k_send.at[d], k_recv.at[d], plane(d)).wait_recv()
        remote(v_slot, v_slot, v_send.at[d], v_recv.at[d], plane(d)).wait_recv()

    def slot_of(ref, b, only_last):
        return ref.at[b, pl.ds(inner - last, last)] if only_last else ref.at[b]

    def lift(b, only_last):
        return (
            remote(slot_of(k_all, b, only_last), slot_of(k_all, b + 1, only_last), kz_send.at[b], kz_recv.at[b + 1], above),
            remote(slot_of(v_all, b, only_last), slot_of(v_all, b + 1, only_last), vz_send.at[b], vz_recv.at[b + 1], above),
        )

    def start_lift(b, only_last):
        @pl.when(has_above & (o >= b))
        def _():
            for copy in lift(b, only_last):
                copy.start()

    def got_lift(b, only_last):
        k_slot, v_slot = slot_of(k_all, b, only_last), slot_of(v_all, b, only_last)
        remote(k_slot, k_slot, kz_send.at[b], kz_recv.at[b], below).wait_recv()
        remote(v_slot, v_slot, vz_send.at[b], vz_recv.at[b], below).wait_recv()

    if back >= 1:
        start_lift(0, back == 1)
    factor = math.log2(math.e) / math.sqrt(width)

    def tile(b, qb, kb, diagonal):
        key_pos = ((o - b) * inner + kb) * tok + lax.broadcasted_iota(jnp.int32, (tok, tok), 0)
        allowed = key_pos >= lo_ref[qb]
        if diagonal:
            allowed &= lax.broadcasted_iota(jnp.int32, (tok, tok), 0) <= lax.broadcasted_iota(
                jnp.int32, (tok, tok), 1
            )
        keys_here, values_here = k_all[b, kb], v_all[b, kb]
        raw = [
            jnp.dot(keys_here, q_all[qb, :, r * tok : (r + 1) * tok], preferred_element_type=jnp.float32)
            for r in range(group)
        ]
        for r in range(group):
            cols = pl.ds(r * tok, tok)
            scores = jnp.where(allowed, raw[r] * factor, -1e30)
            old_max = row_max[qb, :, cols]
            new_max = jnp.maximum(old_max, jnp.max(scores, axis=0, keepdims=True))
            weights = jnp.exp2(scores - new_max)
            rescale = jnp.exp2(old_max - new_max)
            row_max[qb, :, cols] = new_max
            row_total[qb, :, cols] = row_total[qb, :, cols] * rescale + jnp.sum(weights, axis=0, keepdims=True)
            acc[qb, :, cols] = acc[qb, :, cols] * rescale + jnp.dot(
                values_here, weights.astype(jnp.bfloat16), preferred_element_type=jnp.float32
            )

    def own_rows(qb, carry):
        tile(0, qb, qb, True)

        def own_keys(kb, inside):
            tile(0, qb, kb, False)
            return inside

        return lax.fori_loop(0, qb, own_keys, carry)

    own_rows(i, 0)

    @pl.when(o >= 1)
    def _():
        got_lift(1, False)

    start_lift(1, False)
    go_up(1, 1)
    for d in range(1, inner):
        q_slot = q_all.at[from_mate(d)]
        remote(q_slot, q_slot, q_send.at[d], q_recv.at[d], plane(d)).wait_recv()
        own_rows(from_mate(d), 0)
    for c in range(2):
        pass_down(1, c)
    pass_up(1, 0)

    def attend(b, qb):
        def cols(kb, inside):
            tile(b, qb, kb, False)
            return inside

        lax.fori_loop(jnp.maximum(b * inner + qb - span, 0), inner, cols, 0)

    def early_rows(k, carry):
        attend(1, inner - 1 - k)
        return carry

    @pl.when(o >= 1)
    def _():
        lax.fori_loop(0, inner, early_rows, 0)

    @pl.when(o >= 2)
    def _():
        got_lift(2, False)

    start_lift(2, True)
    pass_up(1, 1)

    def a_copy(qb, k):
        slot = a_all.at[qb, i]
        to = {"seq": o * inner + (near_x if k == 0 else near_y)}
        return remote(slot, slot, a_send.at[qb, k], a_recv.at[qb, k], to)

    def send_rows(qb):
        for k in range(2):
            a_copy(qb, k).start()

    def got_near(qb, k):
        slot = a_all.at[qb, near_x if k == 0 else near_y]
        remote(slot, slot, a_send.at[qb, k], a_recv.at[qb, k], plane(1)).wait_recv()

    def relay(qb, k):
        slot = a_all.at[qb, near_x if k == 0 else near_y, pl.ds(k * (tok // 2), tok // 2)]
        to = {"seq": o * inner + (near_y if k == 0 else near_x)}
        return remote(slot, slot, g_send.at[qb, k], g_recv.at[qb, k], to)

    def got_rows(qb):
        for k in range(2):
            slot = a_all.at[qb, inner - 1 - i, pl.ds(k * (tok // 2), tok // 2)]
            remote(slot, slot, g_send.at[qb, k], g_recv.at[qb, k], plane(1)).wait_recv()

    def finish(qb):
        for r in range(group):
            cols = pl.ds(r * tok, tok)
            normal = acc[qb, :, cols] / row_total[qb, :, cols]
            a_all[qb, i, :, r * width : (r + 1) * width] = normal.T.astype(jnp.bfloat16)

    deepest = min(inner, span + inner - back * inner)

    def finish_rows(k, carry):
        qb = inner - 1 - k

        def slots(b, inside):
            attend(b, qb)
            return inside

        lax.fori_loop(2, jnp.minimum(o, back - 1) + 1, slots, 0)
        if back > 1:
            @pl.when((o >= back) & (qb == deepest - 1))
            def _():
                got_lift(back, True)

        if back >= 1:
            @pl.when((o >= back) & (qb < deepest))
            def _():
                attend(back, qb)

        finish(qb)
        send_rows(qb)
        return carry

    lax.fori_loop(0, inner, finish_rows, 0)

    def pass_rows(qb):
        for k in range(2):
            got_near(qb, k)
            relay(qb, k).start()

    pass_rows(inner - 1)
    for c in range(2):
        pass_down(2, c)
    pass_up(2, 0)
    for qb in range(inner - 2, -1, -1):
        pass_rows(qb)
    pass_up(2, 1)

    def multiply(qb, s, cols=slice(None)):
        value = jnp.dot(a_all[qb, 0], w_all[s, 0:part_rows, cols], preferred_element_type=jnp.float32)
        for j in range(1, inner):
            value += jnp.dot(
                a_all[qb, j], w_all[s, j * part_rows : (j + 1) * part_rows, cols], preferred_element_type=jnp.float32
            )
        partial[s, qb, :, cols] = value.astype(jnp.bfloat16)

    def columns(c):
        return pl.ds(0, 2 * half) if c is None else pl.ds(c * half, half)

    def p_copy(s):
        to = s // share
        d = (to + heads - head) % heads
        return remote(
            partial.at[s], peer.at[d, s % share], p_send.at[s], p_recv.at[d, s % share], {"head": to}
        )

    def give(s):
        @pl.when(s // share != head)
        def _():
            p_copy(s).start()

    def c_copy(sl, d):
        return remote(summed.at[sl, mate(d)], result.at[sl, i], c_send.at[sl, d], c_recv.at[sl, d], plane(d))

    def absorb(s):
        @pl.when(s // share == head)
        def _():
            sl = s % share
            for d in range(1, heads):
                slot = peer.at[d, sl]
                remote(slot, slot, p_send.at[s], p_recv.at[d, sl], {"head": (head + d) % heads}).wait_recv()

            def rows(j, carry):
                total = partial[s, j].astype(jnp.float32)
                for d in range(1, heads):
                    total = total + peer[d, sl, j].astype(jnp.float32)
                summed[sl, j] = total.astype(jnp.bfloat16)
                return carry

            lax.fori_loop(0, inner, rows, 0)
            for d in range(1, inner):
                c_copy(sl, d).start()
            result[sl, i] = summed[sl, i]

    def block(k):
        return jnp.where(k == 0, inner - 1 - i, jnp.where(k == 1, near_x, jnp.where(k == 2, near_y, i)))

    def far_give(s, c, k):
        to = s // share
        d = (to + heads - head) % heads
        cols = columns(c)
        return remote(
            partial.at[s, block(k), :, cols], peer.at[d, s % share, block(k), :, cols],
            hp_send.at[c, k], hp_recv.at[c, k], {"head": to},
        )

    def far_copy(s, c, k):
        sl, cols = s % share, columns(c)
        return remote(
            summed.at[sl, block(k), :, cols], result.at[sl, i, :, cols],
            hc_send.at[c, k], hc_recv.at[c, k], {"seq": o * inner + block(k)},
        )

    def far_absorb(s, c, k):
        sl, cols, qb = s % share, columns(c), block(k)
        total = partial[s, qb, :, cols].astype(jnp.float32)
        for d in range(1, heads):
            slot = peer.at[d, sl, qb, :, cols]
            remote(slot, slot, hp_send.at[c, k], hp_recv.at[c, k], {"head": (head + d) % heads}).wait_recv()
            total = total + peer[d, sl, qb, :, cols].astype(jnp.float32)
        total = total.astype(jnp.bfloat16)

        @pl.when(k < inner - 1)
        def _():
            summed[sl, qb, :, cols] = total
            far_copy(s, c, k).start()

        @pl.when(k == inner - 1)
        def _():
            result[sl, i, :, cols] = total

    def near(t, act):
        @pl.when(o - t >= 0)
        def _():
            act(jnp.maximum(o - t, 0))

        @pl.when((o + t < outer) & (t > 0))
        def _():
            act(jnp.minimum(o + t, outer - 1))

    near_count = max(outer - 1, 1)

    def early_blocks(k, carry):
        qb = inner - 1 - k
        got_rows(qb)

        def shards(t, inside):
            near(t, lambda s: multiply(qb, s))
            return inside

        lax.fori_loop(0, near_count, shards, 0)
        return carry

    lax.fori_loop(0, inner - 1, early_blocks, 0)
    got_rows(0)

    def final_block(t, carry):
        def act(s):
            multiply(0, s)
            give(s)

        near(t, act)

        @pl.when(t >= 1)
        def _():
            near(t - 1, absorb)

        return carry

    lax.fori_loop(0, near_count, final_block, 0)
    near(near_count - 1, absorb)
    for c in range(2):
        got_down(outer - 1, c)
        got_up(outer - 1, c)

        def far(s):
            def rows(k, carry):
                @pl.when(k < inner)
                def _():
                    multiply(block(k), s, columns(c))

                @pl.when((k < inner) & (s // share != head))
                def _():
                    far_give(s, c, k).start()

                @pl.when((k >= 1) & (s // share == head))
                def _():
                    far_absorb(s, c, k - 1)

                return carry

            lax.fori_loop(0, inner + 1, rows, 0)

        near(outer - 1, far)

    def is_far(s):
        return (s - o == outer - 1) | (o - s == outer - 1)

    for sl in range(share):
        @pl.when(is_far(head * share + sl))
        def _():
            for c in range(2):
                for k in range(inner - 1):
                    slot = result.at[sl, block(k), :, columns(c)]
                    remote(slot, slot, hc_send.at[c, k], hc_recv.at[c, k], plane(1)).wait_recv()

        @pl.when(jnp.logical_not(is_far(head * share + sl)))
        def _():
            for d in range(1, inner):
                slot = result.at[sl, from_mate(d)]
                remote(slot, slot, c_send.at[sl, d], c_recv.at[sl, d], plane(d)).wait_recv()

    wide = out_ref.shape[1] // (share * inner)
    for s in range(share):
        for j in range(inner):
            out_ref[:, (s * inner + j) * wide : (s * inner + j + 1) * wide] = result[s, j]

    for d in range(1, inner):
        for copy in kv_copies(d):
            copy.wait_send()
        q_copy(d).wait_send()

    for sl in range(share):
        @pl.when(is_far(head * share + sl))
        def _():
            for c in range(2):
                for k in range(inner - 1):
                    far_copy(head * share + sl, c, k).wait_send()

        @pl.when(jnp.logical_not(is_far(head * share + sl)))
        def _():
            for d in range(1, inner):
                c_copy(sl, d).wait_send()

    for qb in range(inner):
        for k in range(2):
            a_copy(qb, k).wait_send()
            relay(qb, k).wait_send()

    def given(s, carry):
        @pl.when((s // share != head) & is_far(s))
        def _():
            for c in range(2):
                for k in range(inner):
                    far_give(s, c, k).wait_send()

        @pl.when((s // share != head) & jnp.logical_not(is_far(s)))
        def _():
            p_copy(s).wait_send()

        return carry

    lax.fori_loop(0, outer, given, 0)

    for b in range(back):
        @pl.when(has_above & (o >= b))
        def _():
            for copy in lift(b, b == back - 1):
                copy.wait_send()

    for t in range(1, outer):
        for c in range(2):
            @pl.when(has_above & (o >= t - 1))
            def _():
                up_copy(t, c).wait_send()

            @pl.when(has_below & (o + t - 1 < outer))
            def _():
                down_copy(t, c).wait_send()


def body(queries, keys, values, out_weight, doc_lengths):
    tok, heads_here, width = queries.shape
    inner = keys.shape[1]
    group = heads_here // inner
    count = lax.axis_size("seq")
    heads = lax.axis_size("head")
    outer = count // inner
    span = count // 2 + 1
    plane_rows = inner * tok
    reach = span * tok - 1
    back = min(outer - 1, -(-reach // plane_rows))
    last = min(inner, -(-(reach - (back - 1) * plane_rows) // tok))
    share = outer // heads
    depth, wide = out_weight.shape

    positions = (lax.axis_index("seq") // inner) * plane_rows + jnp.arange(plane_rows, dtype=jnp.int32)
    ends = jnp.cumsum(doc_lengths)
    starts = jnp.max(jnp.where(ends[None, :] <= positions[:, None], ends[None, :], 0), axis=1)
    starts = starts.reshape(inner, 1, tok)

    bf16, f32 = jnp.bfloat16, jnp.float32
    dma = pltpu.SemaphoreType.DMA
    scratch = [
        pltpu.VMEM((inner, width, group * tok), bf16),
        pltpu.VMEM((inner, tok, width), bf16),
        pltpu.VMEM((inner, width, tok), bf16),
        pltpu.VMEM((inner, width, group * tok), bf16),
        pltpu.VMEM((back + 1, inner, tok, width), bf16),
        pltpu.VMEM((back + 1, inner, width, tok), bf16),
        pltpu.VMEM((outer, depth, wide), bf16),
        pltpu.VMEM((inner, inner, tok, group * width), bf16),
        pltpu.VMEM((inner, width, group * tok), f32),
        pltpu.VMEM((inner, 1, group * tok), f32),
        pltpu.VMEM((inner, 1, group * tok), f32),
        pltpu.VMEM((outer, inner, tok, wide), bf16),
        pltpu.VMEM((heads, share, inner, tok, wide), bf16),
        pltpu.VMEM((share, inner, tok, wide), bf16),
        pltpu.VMEM((share, inner, tok, wide), bf16),
    ]
    scratch += [dma((inner,))] * 6 + [dma((back + 1,))] * 4 + [dma((outer,))] * 4
    scratch += [dma((inner, inner))] * 2 + [dma((outer,)), dma((heads, share))] + [dma((share, inner))] * 2 + [dma((4,))]
    shape = (inner, outer, heads, group, back, span, last)
    vmem = pl.BlockSpec(memory_space=pltpu.VMEM)
    run, last_in, last_spec, first_spec = kernel, starts, vmem, vmem
    if inner == 4 and outer == 4 and back == 3:
        run, last_in, last_spec = square_kernel, doc_lengths, pl.BlockSpec(memory_space=pltpu.SMEM)
        ins = [pltpu.VMEM(a.shape, bf16) for a in (queries, keys, values, out_weight)]
        scratch = ins + [pltpu.VMEM((inner, 1, tok), jnp.int32)] + scratch[:15]
        scratch += [dma((inner,))] * 6 + [dma((back + 1,))] * 4 + [dma((outer, 2))] * 4
        scratch += [dma((inner, 2))] * 4 + [dma((outer,)), dma((heads, share))] + [dma((share, inner))] * 2
        scratch += [dma((2, inner))] * 4 + [dma((4,)), dma((4,))]
        first_spec = pl.BlockSpec(memory_space=pl.ANY)
    return pl.pallas_call(
        functools.partial(run, shape),
        out_shape=pltpu.VMEM((tok, share * inner * wide), bf16),
        in_specs=[first_spec] * 4 + [last_spec],
        out_specs=vmem,
        scratch_shapes=scratch,
        compiler_params=pltpu.CompilerParams(
            collective_id=0, has_side_effects=True, vmem_limit_bytes=60 * 1024 * 1024
        ),
    )(queries, keys, values, out_weight, last_in)


def solution(mesh):
    placed = (
        P("seq", "head", None),
        P("seq", "head", None),
        P("seq", "head", None),
        P("head", "seq"),
        P(),
    )
    return jax.shard_map(
        body, mesh=mesh, in_specs=placed, out_specs=P("seq", "head"), check_vma=False
    )
```

```python
import functools
import math

import jax
import jax.numpy as jnp
from jax import lax
from jax.experimental import pallas as pl
from jax.experimental.pallas import tpu as pltpu
from jax.sharding import PartitionSpec as P

MESH = pl.DeviceIdType.MESH


def kernel(
    shape,
    q_in, k_in, v_in, w_ref, lo_ref, out_ref,
    q_ref, k_ref, v_ref,
    q_all, k_all, v_all, w_all, a_all, acc, row_max, row_total, partial, peer, summed, result,
    q_send, q_recv, k_send, k_recv, v_send, v_recv, kz_send, kz_recv, vz_send, vz_recv,
    up_send, up_recv, down_send, down_recv, a_send, a_recv, p_send, p_recv, c_send, c_recv, local_sem,
):
    inner, outer, heads, group, back, span, last = shape
    tok, width = k_in.shape[0], k_in.shape[2]
    part_rows = group * width
    share = outer // heads
    seq, head = lax.axis_index("seq"), lax.axis_index("head")
    o, i = seq // inner, seq % inner

    def remote(src, dst, send, recv, device):
        return pltpu.make_async_remote_copy(
            src_ref=src, dst_ref=dst, send_sem=send, recv_sem=recv, device_id=device, device_id_type=MESH
        )

    def mate(d):
        return (i + d) % inner

    def plane(d):
        return {"seq": o * inner + mate(d)}

    above, below = {"seq": jnp.minimum(seq + inner, outer * inner - 1)}, {"seq": jnp.maximum(seq - inner, 0)}
    has_above, has_below = o + 1 < outer, o >= 1

    barrier = pltpu.get_barrier_semaphore()
    for d in range(1, inner):
        pl.semaphore_signal(barrier, inc=1, device_id=plane(d), device_id_type=MESH)
    for d in range(1, heads):
        pl.semaphore_signal(barrier, inc=1, device_id={"head": (head + d) % heads}, device_id_type=MESH)

    @pl.when(has_above)
    def _():
        pl.semaphore_signal(barrier, inc=1, device_id=above, device_id_type=MESH)

    @pl.when(has_below)
    def _():
        pl.semaphore_signal(barrier, inc=1, device_id=below, device_id_type=MESH)

    pl.semaphore_wait(
        barrier, inner - 1 + heads - 1 + has_above.astype(jnp.int32) + has_below.astype(jnp.int32)
    )

    def kv_copies(d):
        return (
            remote(k_ref.at[mate(d)], k_all.at[0, i], k_send.at[d], k_recv.at[d], plane(d)),
            remote(v_ref.at[mate(d)], v_all.at[0, i], v_send.at[d], v_recv.at[d], plane(d)),
        )

    def q_copy(d):
        return remote(q_ref.at[mate(d)], q_all.at[i], q_send.at[d], q_recv.at[d], plane(d))

    def up_copy(t, first):
        return remote(
            w_ref if first else w_all.at[jnp.maximum(o - t + 1, 0)],
            w_all.at[jnp.maximum(o - t + 1, 0)], up_send.at[t], up_recv.at[t], above,
        )

    def down_copy(t, first):
        return remote(
            w_ref if first else w_all.at[jnp.minimum(o + t - 1, outer - 1)],
            w_all.at[jnp.minimum(o + t - 1, outer - 1)], down_send.at[t], down_recv.at[t], below,
        )

    def got_up(t):
        @pl.when(o >= t)
        def _():
            slot = w_all.at[jnp.maximum(o - t, 0)]
            remote(slot, slot, up_send.at[t], up_recv.at[t], below).wait_recv()

    def got_down(t):
        @pl.when(o + t < outer)
        def _():
            slot = w_all.at[jnp.minimum(o + t, outer - 1)]
            remote(slot, slot, down_send.at[t], down_recv.at[t], above).wait_recv()

    def go_up(t, first=False):
        @pl.when(has_above & (o >= t - 1))
        def _():
            up_copy(t, first).start()

    def go_down(t, first=False):
        @pl.when(has_below & (o + t - 1 < outer))
        def _():
            down_copy(t, first).start()

    if outer > 1:
        go_up(1, True)
        go_down(1, True)
    k_ref[...] = jnp.swapaxes(k_in[...], 0, 1)
    by_head = jnp.swapaxes(v_in[...], 0, 1)
    for j in range(inner):
        v_ref[j] = by_head[j].T
    by_head = jnp.swapaxes(q_in[...], 0, 1)
    for j in range(inner * group):
        q_ref[j // group, :, (j % group) * tok : (j % group + 1) * tok] = by_head[j].T
    for d in range(1, inner):
        for copy in kv_copies(d):
            copy.start()
    for d in range(1, inner):
        q_copy(d).start()

    locals_ = [
        pltpu.make_async_copy(q_ref.at[i], q_all.at[i], local_sem.at[0]),
        pltpu.make_async_copy(k_ref.at[i], k_all.at[0, i], local_sem.at[1]),
        pltpu.make_async_copy(v_ref.at[i], v_all.at[0, i], local_sem.at[2]),
        pltpu.make_async_copy(w_ref, w_all.at[o], local_sem.at[3]),
    ]
    for copy in locals_:
        copy.start()
    for copy in locals_:
        copy.wait()

    def from_mate(d):
        return (i + inner - d) % inner

    for d in range(1, inner):
        k_slot, v_slot = k_all.at[0, from_mate(d)], v_all.at[0, from_mate(d)]
        remote(k_slot, k_slot, k_send.at[d], k_recv.at[d], plane(d)).wait_recv()
        remote(v_slot, v_slot, v_send.at[d], v_recv.at[d], plane(d)).wait_recv()

    def slot_of(ref, b, only_last):
        return ref.at[b, pl.ds(inner - last, last)] if only_last else ref.at[b]

    def lift(b, only_last):
        return (
            remote(slot_of(k_all, b, only_last), slot_of(k_all, b + 1, only_last), kz_send.at[b], kz_recv.at[b + 1], above),
            remote(slot_of(v_all, b, only_last), slot_of(v_all, b + 1, only_last), vz_send.at[b], vz_recv.at[b + 1], above),
        )

    def start_lift(b, only_last):
        @pl.when(has_above & (o >= b))
        def _():
            for copy in lift(b, only_last):
                copy.start()

    def got_lift(b, only_last):
        k_slot, v_slot = slot_of(k_all, b, only_last), slot_of(v_all, b, only_last)
        remote(k_slot, k_slot, kz_send.at[b], kz_recv.at[b], below).wait_recv()
        remote(v_slot, v_slot, vz_send.at[b], vz_recv.at[b], below).wait_recv()

    if back >= 1:
        start_lift(0, back == 1)
    row_max[...] = jnp.full(row_max.shape, -1e30, jnp.float32)
    row_total[...] = jnp.zeros(row_total.shape, jnp.float32)
    acc[...] = jnp.zeros(acc.shape, jnp.float32)
    factor = math.log2(math.e) / math.sqrt(width)

    def tile(b, qb, kb, diagonal):
        key_pos = ((o - b) * inner + kb) * tok + lax.broadcasted_iota(jnp.int32, (tok, tok), 0)
        allowed = key_pos >= lo_ref[qb]
        if diagonal:
            allowed &= lax.broadcasted_iota(jnp.int32, (tok, tok), 0) <= lax.broadcasted_iota(
                jnp.int32, (tok, tok), 1
            )
        keys_here, values_here = k_all[b, kb], v_all[b, kb]
        raw = [
            jnp.dot(keys_here, q_all[qb, :, r * tok : (r + 1) * tok], preferred_element_type=jnp.float32)
            for r in range(group)
        ]
        for r in range(group):
            cols = pl.ds(r * tok, tok)
            scores = jnp.where(allowed, raw[r] * factor, -1e30)
            old_max = row_max[qb, :, cols]
            new_max = jnp.maximum(old_max, jnp.max(scores, axis=0, keepdims=True))
            weights = jnp.exp2(scores - new_max)
            rescale = jnp.exp2(old_max - new_max)
            row_max[qb, :, cols] = new_max
            row_total[qb, :, cols] = row_total[qb, :, cols] * rescale + jnp.sum(weights, axis=0, keepdims=True)
            acc[qb, :, cols] = acc[qb, :, cols] * rescale + jnp.dot(
                values_here, weights.astype(jnp.bfloat16), preferred_element_type=jnp.float32
            )

    def own_rows(qb, carry):
        tile(0, qb, qb, True)

        def own_keys(kb, inside):
            tile(0, qb, kb, False)
            return inside

        return lax.fori_loop(0, qb, own_keys, carry)

    own_rows(i, 0)
    for d in range(1, inner):
        q_slot = q_all.at[from_mate(d)]
        remote(q_slot, q_slot, q_send.at[d], q_recv.at[d], plane(d)).wait_recv()
        own_rows(from_mate(d), 0)

    def attend(b, qb):
        def cols(kb, inside):
            tile(b, qb, kb, False)
            return inside

        lax.fori_loop(jnp.maximum(b * inner + qb - span, 0), inner, cols, 0)

    def middle(b):
        @pl.when(o >= b)
        def _():
            got_lift(b, False)

        @pl.when(has_above & (o >= b))
        def _():
            for copy in lift(b, False):
                copy.start()

    if outer > 1:
        got_down(1)
    if outer > 2:
        go_down(2)
    def whole_slot(b, carry):
        middle(b)
        return carry

    if back > 2:
        middle(1)
    elif back == 2:
        @pl.when(o >= 1)
        def _():
            got_lift(1, False)

        start_lift(1, True)
    elif back == 1:
        @pl.when(o >= 1)
        def _():
            got_lift(1, True)
    early = inner // 2 if back > 1 else 0

    def early_rows(qb, carry):
        attend(1, qb)
        return carry

    if early:
        @pl.when(o >= 1)
        def _():
            lax.fori_loop(inner - early, inner, early_rows, 0)

    if back > 2:
        lax.fori_loop(2, back - 1, whole_slot, 0)

        @pl.when(o >= back - 1)
        def _():
            got_lift(back - 1, False)

        start_lift(back - 1, True)
    if outer > 1:
        got_up(1)
    if outer > 2:
        go_up(2)

    def a_copy(qb, d):
        slot = a_all.at[qb, i]
        return remote(slot, slot, a_send.at[qb, d], a_recv.at[qb, d], plane(d))

    def send_rows(qb):
        for d in range(1, inner):
            a_copy(qb, d).start()

    def finish(qb):
        for r in range(group):
            cols = pl.ds(r * tok, tok)
            normal = acc[qb, :, cols] / row_total[qb, :, cols]
            a_all[qb, i, :, r * width : (r + 1) * width] = normal.T.astype(jnp.bfloat16)

    deepest = min(inner, span + inner - back * inner)

    def finish_rows(k, carry):
        qb = inner - 1 - k

        def slots(b, inside):
            attend(b, qb)
            return inside

        lax.fori_loop(jnp.where(k < early, 2, 1), jnp.minimum(o, back - 1) + 1, slots, 0)
        if back > 1:
            @pl.when((o >= back) & (qb == deepest - 1))
            def _():
                got_lift(back, True)

        if back >= 1:
            @pl.when((o >= back) & (qb < deepest))
            def _():
                attend(back, qb)

        finish(qb)
        send_rows(qb)
        return carry

    lax.fori_loop(0, inner, finish_rows, 0)

    def hop(t, carry):
        got_down(t - 1)
        go_down(t)
        got_up(t - 1)
        go_up(t)
        return carry

    if outer > 3:
        got_down(2)
        go_down(3)
        got_up(2)
        go_up(3)
        lax.fori_loop(4, outer, hop, 0)
    def multiply(qb, s):
        value = jnp.dot(a_all[qb, 0], w_all[s, 0:part_rows, :], preferred_element_type=jnp.float32)
        for j in range(1, inner):
            value += jnp.dot(
                a_all[qb, j], w_all[s, j * part_rows : (j + 1) * part_rows, :], preferred_element_type=jnp.float32
            )
        partial[s, qb] = value.astype(jnp.bfloat16)

    def p_copy(s):
        to = s // share
        d = (to + heads - head) % heads
        return remote(
            partial.at[s], peer.at[d, s % share], p_send.at[s], p_recv.at[d, s % share], {"head": to}
        )

    def give(s):
        @pl.when(s // share != head)
        def _():
            p_copy(s).start()

    def c_copy(sl, d):
        return remote(summed.at[sl, mate(d)], result.at[sl, i], c_send.at[sl, d], c_recv.at[sl, d], plane(d))

    def absorb(s):
        @pl.when(s // share == head)
        def _():
            sl = s % share
            for d in range(1, heads):
                slot = peer.at[d, sl]
                remote(slot, slot, p_send.at[s], p_recv.at[d, sl], {"head": (head + d) % heads}).wait_recv()

            def rows(j, carry):
                total = partial[s, j].astype(jnp.float32)
                for d in range(1, heads):
                    total = total + peer[d, sl, j].astype(jnp.float32)
                summed[sl, j] = total.astype(jnp.bfloat16)
                return carry

            lax.fori_loop(0, inner, rows, 0)
            for d in range(1, inner):
                c_copy(sl, d).start()
            result[sl, i] = summed[sl, i]

    def near(t, act):
        @pl.when(o - t >= 0)
        def _():
            act(jnp.maximum(o - t, 0))

        @pl.when((o + t < outer) & (t > 0))
        def _():
            act(jnp.minimum(o + t, outer - 1))

    near_count = max(outer - 1, 1)

    def got_rows(qb):
        for d in range(1, inner):
            slot = a_all.at[qb, from_mate(d)]
            remote(slot, slot, a_send.at[qb, d], a_recv.at[qb, d], plane(d)).wait_recv()

    def early_blocks(k, carry):
        qb = inner - 1 - k
        got_rows(qb)

        def shards(t, inside):
            near(t, lambda s: multiply(qb, s))
            return inside

        lax.fori_loop(0, near_count, shards, 0)
        return carry

    lax.fori_loop(0, inner - 1, early_blocks, 0)
    got_rows(0)

    def final_block(t, carry):
        def act(s):
            multiply(0, s)
            give(s)

        near(t, act)

        @pl.when(t >= 1)
        def _():
            near(t - 1, absorb)

        return carry

    lax.fori_loop(0, near_count, final_block, 0)
    near(near_count - 1, absorb)
    if outer > 1:
        if outer > 2:
            got_down(outer - 1)
            got_up(outer - 1)

        def far(s):
            def rows(qb, carry):
                multiply(qb, s)
                return carry

            lax.fori_loop(0, inner, rows, 0)
            give(s)

        near(outer - 1, far)
        near(outer - 1, absorb)
    for sl in range(share):
        for d in range(1, inner):
            slot = result.at[sl, from_mate(d)]
            remote(slot, slot, c_send.at[sl, d], c_recv.at[sl, d], plane(d)).wait_recv()
    wide = out_ref.shape[1] // (share * inner)
    for s in range(share):
        for j in range(inner):
            out_ref[:, (s * inner + j) * wide : (s * inner + j + 1) * wide] = result[s, j]

    for d in range(1, inner):
        for copy in kv_copies(d):
            copy.wait_send()
        q_copy(d).wait_send()
        for qb in range(inner):
            a_copy(qb, d).wait_send()
        for sl in range(share):
            c_copy(sl, d).wait_send()

    def given(s, carry):
        @pl.when(s // share != head)
        def _():
            p_copy(s).wait_send()

        return carry

    lax.fori_loop(0, outer, given, 0)

    def lift_done(b, only_last):
        @pl.when(has_above & (o >= b))
        def _():
            for copy in lift(b, only_last):
                copy.wait_send()

    if back > 1:
        def lift_sent(b, carry):
            lift_done(b, False)
            return carry

        lax.fori_loop(0, back - 1, lift_sent, 0)
    if back >= 1:
        lift_done(back - 1, True)

    def hop_sent(t, first):
        @pl.when(has_above & (o >= t - 1))
        def _():
            up_copy(t, first).wait_send()

        @pl.when(has_below & (o + t - 1 < outer))
        def _():
            down_copy(t, first).wait_send()

    def later_sent(t, carry):
        hop_sent(t, False)
        return carry

    if outer > 1:
        hop_sent(1, True)
        lax.fori_loop(2, outer, later_sent, 0)


def square_kernel(
    shape,
    q_hbm, k_hbm, v_hbm, w_hbm, doc_ref, out_ref,
    q_in, k_in, v_in, w_ref, lo_ref,
    q_ref, k_ref, v_ref,
    q_all, k_all, v_all, w_all, a_all, acc, row_max, row_total, partial, peer, summed, result, ahead,
    q_send, q_recv, k_send, k_recv, v_send, v_recv, kz_send, kz_recv, vz_send, vz_recv,
    up_send, up_recv, down_send, down_recv, a_send, a_recv, g_send, g_recv, p_send, p_recv, c_send, c_recv,
    hp_send, hp_recv, hc_send, hc_recv, in_sem, local_sem,
):
    inner, outer, heads, group, back, span, last = shape
    tok, width = k_in.shape[0], k_in.shape[2]
    part_rows = group * width
    share = outer // heads
    seq, head = lax.axis_index("seq"), lax.axis_index("head")
    o, i = seq // inner, seq % inner
    ix, iy = i % 2, i // 2
    near_x, near_y = iy * 2 + 1 - ix, (1 - iy) * 2 + ix
    half = w_ref.shape[1] // 2

    def remote(src, dst, send, recv, device):
        return pltpu.make_async_remote_copy(
            src_ref=src, dst_ref=dst, send_sem=send, recv_sem=recv, device_id=device, device_id_type=MESH
        )

    def mate(d):
        return (i + d) % inner

    def plane(d):
        return {"seq": o * inner + mate(d)}

    above, below = {"seq": jnp.minimum(seq + inner, outer * inner - 1)}, {"seq": jnp.maximum(seq - inner, 0)}
    has_above, has_below = o + 1 < outer, o >= 1

    fetch_w, fetch_k, fetch_v, fetch_q = (
        pltpu.make_async_copy(src, dst, in_sem.at[j])
        for j, (src, dst) in enumerate(((w_hbm, w_ref), (k_hbm, k_in), (v_hbm, v_in), (q_hbm, q_in)))
    )
    for fetch in (fetch_w, fetch_k, fetch_v, fetch_q):
        fetch.start()

    barrier = pltpu.get_barrier_semaphore()
    for d in range(1, inner):
        pl.semaphore_signal(barrier, inc=1, device_id=plane(d), device_id_type=MESH)
    for d in range(1, heads):
        pl.semaphore_signal(barrier, inc=1, device_id={"head": (head + d) % heads}, device_id_type=MESH)

    @pl.when(has_above)
    def _():
        pl.semaphore_signal(barrier, inc=1, device_id=above, device_id_type=MESH)

    @pl.when(has_below)
    def _():
        pl.semaphore_signal(barrier, inc=1, device_id=below, device_id_type=MESH)

    pl.semaphore_wait(
        barrier, inner - 1 + heads - 1 + has_above.astype(jnp.int32) + has_below.astype(jnp.int32)
    )

    def kv_copies(d):
        return (
            remote(k_ref.at[mate(d)], k_all.at[0, i], k_send.at[d], k_recv.at[d], plane(d)),
            remote(v_ref.at[mate(d)], v_all.at[0, i], v_send.at[d], v_recv.at[d], plane(d)),
        )

    def q_copy(d):
        return remote(q_ref.at[mate(d)], q_all.at[i], q_send.at[d], q_recv.at[d], plane(d))

    def slot_up(t, c):
        return w_all.at[jnp.maximum(o - t, 0), :, pl.ds(c * half, half)]

    def slot_down(t, c):
        return w_all.at[jnp.minimum(o + t, outer - 1), :, pl.ds(c * half, half)]

    rows_half = w_ref.shape[0] // 2

    def tops(slot, t, r, send, recv, to):
        there = slot(t - 1, 1).at[pl.ds(r * rows_half, rows_half)]
        k = t * (1 - r)
        return remote(there, there, send.at[k, 1], recv.at[k, 1], to)

    def last_up(r):
        return tops(slot_up, outer - 1, r, up_send, up_recv, above)

    def last_down(r):
        return tops(slot_down, outer - 1, r, down_send, down_recv, below)

    def got_last(r):
        k = (outer - 1) * (1 - r)
        for gone, slot, send, recv, by in (
            (o >= outer - 1, slot_up, up_send, up_recv, below),
            (o + outer - 1 < outer, slot_down, down_send, down_recv, above),
        ):
            @pl.when(gone)
            def _():
                here = slot(outer - 1, 1).at[pl.ds(r * rows_half, rows_half)]
                remote(here, here, send.at[k, 1], recv.at[k, 1], by).wait_recv()

    def up_copy(t, c):
        src = w_ref.at[:, pl.ds(c * half, half)] if t == 1 else slot_up(t - 1, c)
        return remote(src, slot_up(t - 1, c), up_send.at[t, c], up_recv.at[t, c], above)

    def down_copy(t, c):
        src = w_ref.at[:, pl.ds(c * half, half)] if t == 1 else slot_down(t - 1, c)
        return remote(src, slot_down(t - 1, c), down_send.at[t, c], down_recv.at[t, c], below)

    def got_up(t, c):
        @pl.when(o >= t)
        def _():
            remote(slot_up(t, c), slot_up(t, c), up_send.at[t, c], up_recv.at[t, c], below).wait_recv()

    def got_down(t, c):
        @pl.when(o + t < outer)
        def _():
            remote(slot_down(t, c), slot_down(t, c), down_send.at[t, c], down_recv.at[t, c], above).wait_recv()

    def go_up(t, c):
        @pl.when(has_above & (o >= t - 1))
        def _():
            if t == outer - 1 and c == 1:
                for r in range(2):
                    last_up(r).start()
            else:
                up_copy(t, c).start()

    def go_down(t, c):
        @pl.when(has_below & (o + t - 1 < outer))
        def _():
            if t == outer - 1 and c == 1:
                for r in range(2):
                    last_down(r).start()
            else:
                down_copy(t, c).start()

    def pass_up(t, c):
        got_up(t, c)
        go_up(t + 1, c)

    def pass_down(t, c):
        got_down(t, c)
        go_down(t + 1, c)

    if outer > 1:
        fetch_w.wait()
        go_up(1, 0)
        go_down(1, 0)
        go_down(1, 1)
    fetch_k.wait()
    k_ref[...] = jnp.swapaxes(k_in[...], 0, 1)
    fetch_v.wait()
    by_head = jnp.swapaxes(v_in[...], 0, 1)
    for j in range(inner):
        v_ref[j] = by_head[j].T
    for d in range(1, inner):
        for copy in kv_copies(d):
            copy.start()
    fetch_q.wait()
    by_head = jnp.swapaxes(q_in[...], 0, 1)
    for j in range(inner * group):
        q_ref[j // group, :, (j % group) * tok : (j % group + 1) * tok] = by_head[j].T
    for d in range(1, inner):
        q_copy(d).start()

    locals_ = [
        pltpu.make_async_copy(q_ref.at[i], q_all.at[i], local_sem.at[0]),
        pltpu.make_async_copy(k_ref.at[i], k_all.at[0, i], local_sem.at[1]),
        pltpu.make_async_copy(v_ref.at[i], v_all.at[0, i], local_sem.at[2]),
        pltpu.make_async_copy(w_ref, w_all.at[o], local_sem.at[3]),
    ]
    for copy in locals_:
        copy.start()
    row_max[...] = jnp.full(row_max.shape, -1e30, jnp.float32)
    row_total[...] = jnp.zeros(row_total.shape, jnp.float32)
    acc[...] = jnp.zeros(acc.shape, jnp.float32)
    ends = [doc_ref[0]]
    for j in range(1, doc_ref.shape[0]):
        ends.append(ends[-1] + doc_ref[j])
    for qb in range(inner):
        row = (o * inner + qb) * tok + lax.broadcasted_iota(jnp.int32, (1, tok), 1)
        start = jnp.zeros((1, tok), jnp.int32)
        for end in ends:
            start = jnp.where(row >= end, end, start)
        lo_ref[qb] = start
    for copy in locals_:
        copy.wait()

    def from_mate(d):
        return (i + inner - d) % inner

    for d in range(1, inner):
        k_slot, v_slot = k_all.at[0, from_mate(d)], v_all.at[0, from_mate(d)]
        remote(k_slot, k_slot, k_send.at[d], k_recv.at[d], plane(d)).wait_recv()
        remote(v_slot, v_slot, v_send.at[d], v_recv.at[d], plane(d)).wait_recv()

    def slot_of(ref, b, only_last):
        return ref.at[b, pl.ds(inner - last, last)] if only_last else ref.at[b]

    def lift(b, only_last):
        return (
            remote(slot_of(k_all, b, only_last), slot_of(k_all, b + 1, only_last), kz_send.at[b], kz_recv.at[b + 1], above),
            remote(slot_of(v_all, b, only_last), slot_of(v_all, b + 1, only_last), vz_send.at[b], vz_recv.at[b + 1], above),
        )

    def start_lift(b, only_last):
        @pl.when(has_above & (o >= b))
        def _():
            for copy in lift(b, only_last):
                copy.start()

    def got_lift(b, only_last):
        k_slot, v_slot = slot_of(k_all, b, only_last), slot_of(v_all, b, only_last)
        remote(k_slot, k_slot, kz_send.at[b], kz_recv.at[b], below).wait_recv()
        remote(v_slot, v_slot, vz_send.at[b], vz_recv.at[b], below).wait_recv()

    if back >= 1:
        start_lift(0, back == 1)
    factor = math.log2(math.e) / math.sqrt(width)

    def tile(b, qb, kb, diagonal):
        key_pos = ((o - b) * inner + kb) * tok + lax.broadcasted_iota(jnp.int32, (tok, tok), 0)
        allowed = key_pos >= lo_ref[qb]
        if diagonal:
            allowed &= lax.broadcasted_iota(jnp.int32, (tok, tok), 0) <= lax.broadcasted_iota(
                jnp.int32, (tok, tok), 1
            )
        keys_here, values_here = k_all[b, kb], v_all[b, kb]
        raw = [
            jnp.dot(keys_here, q_all[qb, :, r * tok : (r + 1) * tok], preferred_element_type=jnp.float32)
            for r in range(group)
        ]
        for r in range(group):
            cols = pl.ds(r * tok, tok)
            scores = jnp.where(allowed, raw[r] * factor, -1e30)
            old_max = row_max[qb, :, cols]
            new_max = jnp.maximum(old_max, jnp.max(scores, axis=0, keepdims=True))
            weights = jnp.exp2(scores - new_max)
            rescale = jnp.exp2(old_max - new_max)
            row_max[qb, :, cols] = new_max
            row_total[qb, :, cols] = row_total[qb, :, cols] * rescale + jnp.sum(weights, axis=0, keepdims=True)
            acc[qb, :, cols] = acc[qb, :, cols] * rescale + jnp.dot(
                values_here, weights.astype(jnp.bfloat16), preferred_element_type=jnp.float32
            )

    def own_rows(qb, carry):
        tile(0, qb, qb, True)

        def own_keys(kb, inside):
            tile(0, qb, kb, False)
            return inside

        return lax.fori_loop(0, qb, own_keys, carry)

    own_rows(i, 0)

    @pl.when(o >= 1)
    def _():
        got_lift(1, False)

    start_lift(1, False)
    go_up(1, 1)
    for d in range(1, inner):
        q_slot = q_all.at[from_mate(d)]
        remote(q_slot, q_slot, q_send.at[d], q_recv.at[d], plane(d)).wait_recv()
        own_rows(from_mate(d), 0)
    for c in range(2):
        pass_down(1, c)
    pass_up(1, 0)

    def attend(b, qb):
        def cols(kb, inside):
            tile(b, qb, kb, False)
            return inside

        lax.fori_loop(jnp.maximum(b * inner + qb - span, 0), inner, cols, 0)

    def early_rows(k, carry):
        attend(1, inner - 1 - k)
        return carry

    @pl.when(o >= 1)
    def _():
        lax.fori_loop(0, inner, early_rows, 0)

    @pl.when(o >= 2)
    def _():
        got_lift(2, False)

    start_lift(2, True)
    pass_up(1, 1)

    def a_copy(qb, k):
        slot = a_all.at[qb, i]
        to = {"seq": o * inner + (near_x if k == 0 else near_y)}
        return remote(slot, slot, a_send.at[qb, k], a_recv.at[qb, k], to)

    def send_rows(qb):
        for k in range(2):
            a_copy(qb, k).start()

    def got_near(qb, k):
        slot = a_all.at[qb, near_x if k == 0 else near_y]
        remote(slot, slot, a_send.at[qb, k], a_recv.at[qb, k], plane(1)).wait_recv()

    def relay(qb, k):
        slot = a_all.at[qb, near_x if k == 0 else near_y, pl.ds(k * (tok // 2), tok // 2)]
        to = {"seq": o * inner + (near_y if k == 0 else near_x)}
        return remote(slot, slot, g_send.at[qb, k], g_recv.at[qb, k], to)

    def got_rows(qb):
        for k in range(2):
            slot = a_all.at[qb, inner - 1 - i, pl.ds(k * (tok // 2), tok // 2)]
            remote(slot, slot, g_send.at[qb, k], g_recv.at[qb, k], plane(1)).wait_recv()

    def finish(qb):
        for r in range(group):
            cols = pl.ds(r * tok, tok)
            normal = acc[qb, :, cols] / row_total[qb, :, cols]
            a_all[qb, i, :, r * width : (r + 1) * width] = normal.T.astype(jnp.bfloat16)

    deepest = min(inner, span + inner - back * inner)

    def finish_rows(k, carry):
        qb = inner - 1 - k

        def slots(b, inside):
            attend(b, qb)
            return inside

        lax.fori_loop(2, jnp.minimum(o, back - 1) + 1, slots, 0)
        if back > 1:
            @pl.when((o >= back) & (qb == deepest - 1))
            def _():
                got_lift(back, True)

        if back >= 1:
            @pl.when((o >= back) & (qb < deepest))
            def _():
                attend(back, qb)

        finish(qb)
        send_rows(qb)
        return carry

    lax.fori_loop(0, inner, finish_rows, 0)

    def pass_rows(qb):
        for k in range(2):
            got_near(qb, k)
            relay(qb, k).start()

    pass_rows(inner - 1)
    for c in range(2):
        pass_down(2, c)
    pass_up(2, 0)
    for qb in range(inner - 2, -1, -1):
        pass_rows(qb)
    pass_up(2, 1)

    def product(qb, s, cols, begin, end):
        value = None
        for j in range(begin, end):
            term = jnp.dot(
                a_all[qb, j], w_all[s, j * part_rows : (j + 1) * part_rows, cols], preferred_element_type=jnp.float32
            )
            value = term if value is None else value + term
        return value

    def multiply(qb, s, cols=slice(None)):
        partial[s, qb, :, cols] = product(qb, s, cols, 0, inner).astype(jnp.bfloat16)

    def columns(c):
        return pl.ds(0, 2 * half) if c is None else pl.ds(c * half, half)

    def p_copy(s):
        to = s // share
        d = (to + heads - head) % heads
        return remote(
            partial.at[s], peer.at[d, s % share], p_send.at[s], p_recv.at[d, s % share], {"head": to}
        )

    def give(s):
        @pl.when(s // share != head)
        def _():
            p_copy(s).start()

    def c_copy(sl, d):
        return remote(summed.at[sl, mate(d)], result.at[sl, i], c_send.at[sl, d], c_recv.at[sl, d], plane(d))

    def absorb(s):
        @pl.when(s // share == head)
        def _():
            sl = s % share
            for d in range(1, heads):
                slot = peer.at[d, sl]
                remote(slot, slot, p_send.at[s], p_recv.at[d, sl], {"head": (head + d) % heads}).wait_recv()

            def rows(j, carry):
                total = partial[s, j].astype(jnp.float32)
                for d in range(1, heads):
                    total = total + peer[d, sl, j].astype(jnp.float32)
                summed[sl, j] = total.astype(jnp.bfloat16)
                return carry

            lax.fori_loop(0, inner, rows, 0)
            for d in range(1, inner):
                c_copy(sl, d).start()
            result[sl, i] = summed[sl, i]

    def block(k):
        return jnp.where(k == 0, inner - 1 - i, jnp.where(k == 1, near_x, jnp.where(k == 2, near_y, i)))

    def far_give(s, c, k):
        to = s // share
        d = (to + heads - head) % heads
        cols = columns(c)
        return remote(
            partial.at[s, block(k), :, cols], peer.at[d, s % share, block(k), :, cols],
            hp_send.at[c, k], hp_recv.at[c, k], {"head": to},
        )

    def far_copy(s, c, k):
        sl, cols = s % share, columns(c)
        return remote(
            summed.at[sl, block(k), :, cols], result.at[sl, i, :, cols],
            hc_send.at[c, k], hc_recv.at[c, k], {"seq": o * inner + block(k)},
        )

    def far_absorb(s, c, k):
        sl, cols, qb = s % share, columns(c), block(k)
        total = partial[s, qb, :, cols].astype(jnp.float32)
        for d in range(1, heads):
            slot = peer.at[d, sl, qb, :, cols]
            remote(slot, slot, hp_send.at[c, k], hp_recv.at[c, k], {"head": (head + d) % heads}).wait_recv()
            total = total + peer[d, sl, qb, :, cols].astype(jnp.float32)
        total = total.astype(jnp.bfloat16)

        @pl.when(k < inner - 1)
        def _():
            summed[sl, qb, :, cols] = total
            far_copy(s, c, k).start()

        @pl.when(k == inner - 1)
        def _():
            result[sl, i, :, cols] = total

    def near(t, act):
        @pl.when(o - t >= 0)
        def _():
            act(jnp.maximum(o - t, 0))

        @pl.when((o + t < outer) & (t > 0))
        def _():
            act(jnp.minimum(o + t, outer - 1))

    near_count = max(outer - 1, 1)

    def early_blocks(k, carry):
        qb = inner - 1 - k
        got_rows(qb)

        def shards(t, inside):
            near(t, lambda s: multiply(qb, s))
            return inside

        lax.fori_loop(0, near_count, shards, 0)
        return carry

    lax.fori_loop(0, inner - 1, early_blocks, 0)
    got_rows(0)

    def final_block(t, carry):
        def act(s):
            multiply(0, s)
            give(s)

        near(t, act)

        @pl.when(t >= 1)
        def _():
            near(t - 1, absorb)

        return carry

    lax.fori_loop(0, near_count, final_block, 0)
    near(near_count - 1, absorb)
    for c in range(2):
        if c == 0:
            got_down(outer - 1, c)
            got_up(outer - 1, c)
        else:
            got_last(0)

            def begin(s):
                def rows(k, carry):
                    ahead[k] = product(block(k), s, columns(1), 0, inner // 2)
                    return carry

                lax.fori_loop(0, inner, rows, 0)

            near(outer - 1, begin)
            got_last(1)

        def far(s):
            def rows(k, carry):
                @pl.when(k < inner)
                def _():
                    if c == 0:
                        multiply(block(k), s, columns(c))
                    else:
                        value = ahead[k] + product(block(k), s, columns(c), inner // 2, inner)
                        partial[s, block(k), :, columns(c)] = value.astype(jnp.bfloat16)

                @pl.when((k < inner) & (s // share != head))
                def _():
                    far_give(s, c, k).start()

                @pl.when((k >= 1) & (s // share == head))
                def _():
                    far_absorb(s, c, k - 1)

                return carry

            lax.fori_loop(0, inner + 1, rows, 0)

        near(outer - 1, far)

    def is_far(s):
        return (s - o == outer - 1) | (o - s == outer - 1)

    for sl in range(share):
        @pl.when(is_far(head * share + sl))
        def _():
            for c in range(2):
                for k in range(inner - 1):
                    slot = result.at[sl, block(k), :, columns(c)]
                    remote(slot, slot, hc_send.at[c, k], hc_recv.at[c, k], plane(1)).wait_recv()

        @pl.when(jnp.logical_not(is_far(head * share + sl)))
        def _():
            for d in range(1, inner):
                slot = result.at[sl, from_mate(d)]
                remote(slot, slot, c_send.at[sl, d], c_recv.at[sl, d], plane(d)).wait_recv()

    wide = out_ref.shape[1] // (share * inner)
    for s in range(share):
        for j in range(inner):
            out_ref[:, (s * inner + j) * wide : (s * inner + j + 1) * wide] = result[s, j]

    for d in range(1, inner):
        for copy in kv_copies(d):
            copy.wait_send()
        q_copy(d).wait_send()

    for sl in range(share):
        @pl.when(is_far(head * share + sl))
        def _():
            for c in range(2):
                for k in range(inner - 1):
                    far_copy(head * share + sl, c, k).wait_send()

        @pl.when(jnp.logical_not(is_far(head * share + sl)))
        def _():
            for d in range(1, inner):
                c_copy(sl, d).wait_send()

    for qb in range(inner):
        for k in range(2):
            a_copy(qb, k).wait_send()
            relay(qb, k).wait_send()

    def given(s, carry):
        @pl.when((s // share != head) & is_far(s))
        def _():
            for c in range(2):
                for k in range(inner):
                    far_give(s, c, k).wait_send()

        @pl.when((s // share != head) & jnp.logical_not(is_far(s)))
        def _():
            p_copy(s).wait_send()

        return carry

    lax.fori_loop(0, outer, given, 0)

    for b in range(back):
        @pl.when(has_above & (o >= b))
        def _():
            for copy in lift(b, b == back - 1):
                copy.wait_send()

    for t in range(1, outer):
        for c in range(2):
            @pl.when(has_above & (o >= t - 1))
            def _():
                if t == outer - 1 and c == 1:
                    for r in range(2):
                        last_up(r).wait_send()
                else:
                    up_copy(t, c).wait_send()

            @pl.when(has_below & (o + t - 1 < outer))
            def _():
                if t == outer - 1 and c == 1:
                    for r in range(2):
                        last_down(r).wait_send()
                else:
                    down_copy(t, c).wait_send()


def body(queries, keys, values, out_weight, doc_lengths):
    tok, heads_here, width = queries.shape
    inner = keys.shape[1]
    group = heads_here // inner
    count = lax.axis_size("seq")
    heads = lax.axis_size("head")
    outer = count // inner
    span = count // 2 + 1
    plane_rows = inner * tok
    reach = span * tok - 1
    back = min(outer - 1, -(-reach // plane_rows))
    last = min(inner, -(-(reach - (back - 1) * plane_rows) // tok))
    share = outer // heads
    depth, wide = out_weight.shape

    positions = (lax.axis_index("seq") // inner) * plane_rows + jnp.arange(plane_rows, dtype=jnp.int32)
    ends = jnp.cumsum(doc_lengths)
    starts = jnp.max(jnp.where(ends[None, :] <= positions[:, None], ends[None, :], 0), axis=1)
    starts = starts.reshape(inner, 1, tok)

    bf16, f32 = jnp.bfloat16, jnp.float32
    dma = pltpu.SemaphoreType.DMA
    scratch = [
        pltpu.VMEM((inner, width, group * tok), bf16),
        pltpu.VMEM((inner, tok, width), bf16),
        pltpu.VMEM((inner, width, tok), bf16),
        pltpu.VMEM((inner, width, group * tok), bf16),
        pltpu.VMEM((back + 1, inner, tok, width), bf16),
        pltpu.VMEM((back + 1, inner, width, tok), bf16),
        pltpu.VMEM((outer, depth, wide), bf16),
        pltpu.VMEM((inner, inner, tok, group * width), bf16),
        pltpu.VMEM((inner, width, group * tok), f32),
        pltpu.VMEM((inner, 1, group * tok), f32),
        pltpu.VMEM((inner, 1, group * tok), f32),
        pltpu.VMEM((outer, inner, tok, wide), bf16),
        pltpu.VMEM((heads, share, inner, tok, wide), bf16),
        pltpu.VMEM((share, inner, tok, wide), bf16),
        pltpu.VMEM((share, inner, tok, wide), bf16),
    ]
    scratch += [dma((inner,))] * 6 + [dma((back + 1,))] * 4 + [dma((outer,))] * 4
    scratch += [dma((inner, inner))] * 2 + [dma((outer,)), dma((heads, share))] + [dma((share, inner))] * 2 + [dma((4,))]
    shape = (inner, outer, heads, group, back, span, last)
    vmem = pl.BlockSpec(memory_space=pltpu.VMEM)
    run, last_in, last_spec, first_spec = kernel, starts, vmem, vmem
    if inner == 4 and outer == 4 and back == 3:
        run, last_in, last_spec = square_kernel, doc_lengths, pl.BlockSpec(memory_space=pltpu.SMEM)
        ins = [pltpu.VMEM(a.shape, bf16) for a in (queries, keys, values, out_weight)]
        scratch = ins + [pltpu.VMEM((inner, 1, tok), jnp.int32)] + scratch[:15]
        scratch += [pltpu.VMEM((inner, tok, wide // 2), f32)]
        scratch += [dma((inner,))] * 6 + [dma((back + 1,))] * 4 + [dma((outer, 2))] * 4
        scratch += [dma((inner, 2))] * 4 + [dma((outer,)), dma((heads, share))] + [dma((share, inner))] * 2
        scratch += [dma((2, inner))] * 4 + [dma((4,)), dma((4,))]
        first_spec = pl.BlockSpec(memory_space=pl.ANY)
    return pl.pallas_call(
        functools.partial(run, shape),
        out_shape=pltpu.VMEM((tok, share * inner * wide), bf16),
        in_specs=[first_spec] * 4 + [last_spec],
        out_specs=vmem,
        scratch_shapes=scratch,
        compiler_params=pltpu.CompilerParams(
            collective_id=0, has_side_effects=True, vmem_limit_bytes=60 * 1024 * 1024
        ),
    )(queries, keys, values, out_weight, last_in)


def solution(mesh):
    placed = (
        P("seq", "head", None),
        P("seq", "head", None),
        P("seq", "head", None),
        P("head", "seq"),
        P(),
    )
    return jax.shard_map(
        body, mesh=mesh, in_specs=placed, out_specs=P("seq", "head"), check_vma=False
    )
```
